512 devices in a mesh: gx: 16 (over z, core), gy: 8 (over y), gz: 4 (over x).
Axes of the slice: x: 4, y: 8, z: 8, core: 2. Of those that a mesh axis runs over, the one named last changes fastest.
Arguments:
- points: float32 [16384, 3, 128], P(('gx', 'gy', 'gz'))
- charges: float32 [16384, 128], P(('gx', 'gy', 'gz')), may hold values from -0.6 to 0.6
- interpolant: float32 [16384, 64, 64], P(('gx', 'gy', 'gz')), may hold values from -0.75 to 0.75
- leaf_transfer: float32 [16384, 64, 64], P(('gx', 'gy', 'gz'))
- node_transfer: float32 [512, 9, 64, 64], P(('gx', 'gy', 'gz')), as said below
- node_points: float32 [512, 9, 3, 64], P(('gx', 'gy', 'gz')), as said below
- near_list: int32 [16384, 8], P(('gx', 'gy', 'gz')), may hold values from 0 to 47, as said below
- near_count: int32 [16384], P(('gx', 'gy', 'gz')), may hold values from 1 to 8, as said below
- far_list: int32 [16384, 8], P(('gx', 'gy', 'gz')), may hold values from 0 to 47, as said below
Outputs:
- potential: float32 [16384, 128], P(('gx', 'gy', 'gz'))
The draws below stay inside these ranges and needn't reach their ends.
Inputs may be any that keep to these rules, and one draw needn't show every extreme that they name: `near_list`: entry 0 of the list of a leaf with number i within its device is i + 8; the other entries are distinct positions within 8 of i + 8. `far_list`: distinct positions within 8 of the leaf's own position i + 8, none of them in the leaf's near list. Only the first near_count[g] entries of leaf g's near list are used. `node_transfer`: rows of devices in the same node (k, c) are equal at level k. `node_points`: rows of devices in the same node (k, c) are equal at level k.
All inputs are finite; a program needn't handle non-finite values.
Results may differ from the reference program's by a relative error of at most 0.0003.
Values sent between devices are 32-bit elements; how exact they have to be, the bound alone decides.
No kernel may reach another device: no remote copies, remote signals or barrier semaphores. Data moves between devices by JAX's collectives and lax.ppermute only.
A program may use at most 64 MiB of HBM per device.

```python
import jax
import jax.numpy as jnp
from jax import lax

RANK = 64
PTS = 128
NEAR = 8
FAR = 8
LEAF_DEV = 32
HALO = 8
CLUSTERS = 512
LEAVES = 16384
LEVELS = 9


def morton_cell(index, bit_count):
    coords = [jnp.zeros_like(index), jnp.zeros_like(index), jnp.zeros_like(index)]
    for bit_place in range(bit_count):
        coords[bit_place % 3] = coords[bit_place % 3] + ((index >> bit_place & 1) << bit_place // 3)
    return jnp.stack(coords).astype(jnp.float32)


def draw_points(key, part):
    index = jnp.arange(LEAVES, dtype=jnp.int32)
    cells = morton_cell(index, LEAVES.bit_length() - 1)
    unit = jax.random.uniform(key, (LEAVES, 3, PTS), jnp.float32)
    return cells.T[:, :, None] + 2.0 * unit - 0.5


def node_copies(base):
    device = jnp.arange(CLUSTERS, dtype=jnp.int32)
    layers = []
    for level_index in range(LEVELS):
        first = device >> level_index << level_index
        layers.append(base[level_index][first])
    return jnp.stack(layers, axis=1)


def draw_node_points(key, part):
    total_bits = LEAVES.bit_length() - 1
    leaf_bits = LEAF_DEV.bit_length() - 1
    unit = jax.random.uniform(key, (LEVELS, CLUSTERS, 3, RANK), jnp.float32)
    device = jnp.arange(CLUSTERS, dtype=jnp.int32)
    layers = []
    for level_index in range(LEVELS):
        first = device >> level_index << level_index
        corner = morton_cell(first * LEAF_DEV, total_bits)
        span_bits = level_index + leaf_bits
        extent_list = []
        for axis_pick in range(3):
            bit_total = 0
            for bit_place in range(span_bits):
                if bit_place % 3 == axis_pick:
                    bit_total = bit_total + 1
            side_length = 2 ** bit_total
            extent_list.append(float(side_length))
        extent = jnp.array(extent_list, jnp.float32)
        layers.append(corner.T[:, :, None] + extent[None, :, None] * unit[level_index][first])
    return jnp.stack(layers, axis=1)


def draw_node_transfer(key, part):
    scale = 2.0 ** (-0.25) / RANK ** 0.5
    base = jax.random.normal(key, (LEVELS, CLUSTERS, RANK, RANK), jnp.float32) * scale
    return node_copies(base)


def draw_leaf_transfer(key, part):
    scale = LEAF_DEV ** (-0.25) / RANK ** 0.5
    return jax.random.normal(key, (LEAVES, RANK, RANK), jnp.float32) * scale


def neighbor_table(key):
    subkey = jax.random.fold_in(key, 11)
    spread = 2 * HALO
    scores = jax.random.randint(subkey, (LEAVES, spread), 0, 1 << 20) * spread + jnp.arange(spread, dtype=jnp.int32)[None, :]
    order = jnp.argsort(scores, axis=1, stable=True).astype(jnp.int32)
    offset = jnp.where(order < HALO, order - HALO, order - HALO + 1)
    home = jnp.arange(LEAVES, dtype=jnp.int32) % LEAF_DEV + HALO
    window = home[:, None] + offset
    near_part = jnp.concatenate([home[:, None], window[:, :NEAR - 1]], axis=1)
    far_part = window[:, NEAR - 1:NEAR - 1 + FAR]
    return (near_part, far_part)


def draw_near_list(key, part):
    return neighbor_table(key)[0]


def draw_far_list(key, part):
    return neighbor_table(key)[1]


def draw_near_count(key, part):
    first_key = jax.random.fold_in(key, 3)
    second_key = jax.random.fold_in(key, 5)
    third_key = jax.random.fold_in(key, 9)
    device_level = jax.random.randint(first_key, (CLUSTERS,), 1, NEAR + 1)
    per_leaf = jax.random.randint(second_key, (CLUSTERS, LEAF_DEV), 0, 1 << 20) % device_level[:, None] + 1
    chosen = jax.random.randint(third_key, (), 0, LEAVES)
    counts = per_leaf.reshape(LEAVES)
    return jnp.where(jnp.arange(LEAVES, dtype=jnp.int32) == chosen, NEAR, counts).astype(jnp.int32)


def block_scale(rng, shape, shards, smallest, largest):
    def one(axis_at, shards_of):
        draws = jax.random.uniform(jax.random.fold_in(jax.random.fold_in(rng, 6), axis_at), (shards_of,), jnp.float32, smallest / len(shards), largest / len(shards))
        return jnp.repeat(jnp.exp(draws), shape[axis_at] // shards_of).reshape((-1,) + (1,) * (len(shape) - axis_at - 1))

    factor_of = one(*shards[0])
    for cut in shards[1:]:
        factor_of = factor_of * one(*cut)
    return factor_of


def centred(stream_key, shape, scale, reach, cuts=(), kind=jnp.bfloat16):
    values = scale * jax.random.normal(stream_key, shape, jnp.float32)
    if cuts:
        values = values * block_scale(stream_key, shape, cuts, -0.22, 0.18)
    return jnp.clip(values, -reach, reach).astype(kind)


def setup_inputs(seed: int = 0) -> dict:
    key_of = jax.random.split(jax.random.key(seed), 10)
    return {
        "points": draw_points(jax.random.fold_in(key_of[9], 71), 0),
        "charges": centred(key_of[1], (LEAVES, PTS), 0.1, 0.6, ((0, 512),), jnp.float32),
        "interpolant": centred(key_of[2], (LEAVES, RANK, PTS - RANK), (PTS - RANK) ** -0.5, 0.75, ((0, 512),), jnp.float32),
        "leaf_transfer": draw_leaf_transfer(jax.random.fold_in(key_of[9], 71), 0),
        "node_transfer": draw_node_transfer(jax.random.fold_in(key_of[9], 71), 0),
        "node_points": draw_node_points(jax.random.fold_in(key_of[9], 71), 0),
        "near_list": draw_near_list(jax.random.fold_in(key_of[9], 71), 0),
        "near_count": draw_near_count(jax.random.fold_in(key_of[9], 71), 0),
        "far_list": draw_far_list(jax.random.fold_in(key_of[9], 71), 0),
    }


SOFTENING = 0.0625
HIGHEST = lax.Precision.HIGHEST

def kernel(targets, sources):
    spread = targets[..., :, :, None] - sources[..., :, None, :]
    return lax.rsqrt(lax.optimization_barrier(jnp.sum(spread * spread, axis=-3)) + SOFTENING)

def leaf_terms(window, near_list, near_count, far_list, skeleton_rank):
    leaves = near_list.shape[0]
    margin = (window.shape[0] - leaves) // 2
    targets = window[margin:margin + leaves]
    blocks = leaves // 4

    def block_terms(pieces):
        target_block, near_block, count_block, far_block = pieces
        sources = window[near_block]
        slot_index = jnp.arange(near_block.shape[1], dtype=jnp.int32)
        is_live = slot_index[None, :] < count_block[:, None]
        weights = jnp.where(is_live[:, :, None], sources[:, :, 3, :], 0.0)
        kernel_tiles = kernel(target_block[:, None, 0:3, :], sources[:, :, 0:3, :])
        near_part = jnp.einsum('bmpq,bmq->bp', kernel_tiles, weights, precision=HIGHEST)
        distant = window[far_block]
        coupling = kernel(target_block[:, None, 0:3, :skeleton_rank], distant[:, :, 0:3, :skeleton_rank])
        far_part = jnp.einsum('bmpq,bmq->bp', coupling, distant[:, :, 4, :skeleton_rank], precision=HIGHEST)
        return (near_part, far_part)
    near_part, far_part = lax.map(block_terms, (targets.reshape((blocks, 4) + targets.shape[1:]), near_list.reshape(blocks, 4, near_list.shape[1]), near_count.reshape(blocks, 4), far_list.reshape(blocks, 4, far_list.shape[1])))
    return (near_part.reshape(leaves, near_part.shape[2]), far_part.reshape(leaves, far_part.shape[2]))

def reference(points, charges, interpolant, leaf_transfer, node_transfer, node_points, near_list, near_count, far_list):
    skeleton = charges[:, :RANK] + jnp.einsum('lrp,lp->lr', interpolant, charges[:, RANK:], precision=HIGHEST)
    packed = jnp.concatenate([points, charges[:, None, :], jnp.pad(skeleton, ((0, 0), (0, PTS - RANK)))[:, None, :]], axis=1)
    padded = jnp.pad(packed, ((HALO, HALO), (0, 0), (0, 0)))
    blocks_up = leaf_transfer.reshape(CLUSTERS, LEAF_DEV, RANK, RANK)
    device_skeleton = jnp.einsum('dirc,dir->dc', blocks_up, skeleton.reshape(CLUSTERS, LEAF_DEV, RANK), precision=HIGHEST)
    current = device_skeleton
    couplings = []
    for level_index in range(LEVELS):
        stride = 2 ** level_index
        transfer_rows = node_transfer[::stride, level_index]
        centres = node_points[::stride, level_index]
        count_nodes = current.shape[0]
        swapped = current.reshape(count_nodes // 2, 2, RANK)[:, ::-1].reshape(count_nodes, RANK)
        partner_centres = centres.reshape(count_nodes // 2, 2, 3, RANK)[:, ::-1].reshape(count_nodes, 3, RANK)
        couplings.append(jnp.einsum('nab,nb->na', kernel(centres, partner_centres), swapped, precision=HIGHEST))
        lifted = jnp.einsum('nrc,nr->nc', transfer_rows, current, precision=HIGHEST)
        current = lifted.reshape(count_nodes // 2, 2, RANK).sum(axis=1)
    expansion = couplings[-1]
    for level_index in range(LEVELS - 1, 0, -1):
        stride = 2 ** (level_index - 1)
        transfer_rows = node_transfer[::stride, level_index - 1]
        parents = jnp.repeat(expansion, 2, axis=0)
        expansion = couplings[level_index - 1] + jnp.einsum('nrc,nc->nr', transfer_rows, parents, precision=HIGHEST)
    from_device = jnp.einsum('dirc,dc->dir', blocks_up, expansion, precision=HIGHEST).reshape(LEAVES, RANK)

    def device_terms(device):
        start = (device * LEAF_DEV).astype(jnp.int32)
        window = lax.dynamic_slice_in_dim(padded, start, LEAF_DEV + 2 * HALO, 0)
        near_rows = lax.dynamic_slice_in_dim(near_list, start, LEAF_DEV, 0)
        count_rows = lax.dynamic_slice_in_dim(near_count, start, LEAF_DEV, 0)
        far_rows = lax.dynamic_slice_in_dim(far_list, start, LEAF_DEV, 0)
        return leaf_terms(window, near_rows, count_rows, far_rows, RANK)
    near_part, far_part = lax.map(device_terms, jnp.arange(CLUSTERS, dtype=jnp.int32))
    combined = far_part.reshape(LEAVES, RANK) + from_device
    upper = jnp.einsum('lrp,lr->lp', interpolant, combined, precision=HIGHEST)
    return jnp.concatenate([combined, upper], axis=1) + near_part.reshape(LEAVES, PTS)
```

```python
import jax
import jax.numpy as jnp
from jax import lax
from jax.experimental import pallas as pl
from jax.experimental.pallas import tpu as pltpu
from jax.sharding import PartitionSpec as P


HALO = 8
SOFTENING = 0.0625
AXES = ("gx", "gy", "gz")
INTERPRET = False
CHUNKS = 4


class Layout:
    def __init__(self, nx, ny, nz):
        self.nx, self.ny, self.nz = nx, ny, nz
        self.bx, self.by, self.bz = (n.bit_length() - 1 for n in (nx, ny, nz))
        self.levels = self.bx + self.by + self.bz
        self.core = self.bz + self.by
        self.na = 2 * nz
        self.nb = (nx // 2) * ny
        self.low = list(range(self.bz, self.core))
        self.high = list(range(self.core + 1, self.levels))
        both = self.low + self.high
        self.pairs = [both[i : i + 2] for i in range(0, len(both), 2)]
        self.rows_a = 2 + len(self.pairs)
        self.rows_b = 3

    def device(self, a, b):
        gz, core = a % self.nz, a // self.nz
        gy, up = b % self.ny, b // self.ny
        return ((up * 2 + core) * self.ny + gy) * self.nz + gz

    def groups_a(self):
        return [[self.device(a, b) for a in range(self.na)] for b in range(self.nb)]

    def groups_b(self):
        return [[self.device(a, b) for b in range(self.nb)] for a in range(self.na)]

    def level_a(self, diff):
        if diff == 0:
            return 0
        return self.core if diff >= self.nz else diff.bit_length() - 1

    def level_b(self, diff):
        high, low = diff // self.ny, diff % self.ny
        if high:
            return self.core + high.bit_length()
        return self.bz + low.bit_length() - 1 if low else self.bz

    def place(self):
        gx, gy, gz = (lax.axis_index(name) for name in AXES)
        return (gx % 2) * self.nz + gz, (gx // 2) * self.ny + gy


def eye(rows, lanes):
    r = lax.broadcasted_iota(jnp.int32, (rows, lanes), 0)
    c = lax.broadcasted_iota(jnp.int32, (rows, lanes), 1)
    return r == c % rows


def to_row(col, mask):
    return jnp.sum(jnp.where(mask, col, 0.0), axis=0, keepdims=True)


def side(left, right):
    return jnp.concatenate([left, right], axis=1)


def pre_kernel(
    lay, pts_hbm, q_hbm, p_hbm, e_hbm, w_hbm, t_hbm, pack, lo, hi, send, msg, e_ref, p_ref, pts, q, w_ref, t_ref, sem
):
    leaves, rank = w_ref.shape[0], w_ref.shape[1]
    step = leaves // CHUNKS
    small = [
        pltpu.make_async_copy(src, dst, sem.at[2 * CHUNKS + n])
        for n, (src, dst) in enumerate(((q_hbm, q), (pts_hbm, pts), (e_hbm, e_ref), (p_hbm, p_ref)))
    ]
    small[0].start()
    small[1].start()
    copies = []
    for c in range(CHUNKS):
        part = pl.ds(c * step, step)
        copies.append(
            (
                pltpu.make_async_copy(w_hbm.at[part], w_ref.at[part], sem.at[2 * c]),
                pltpu.make_async_copy(t_hbm.at[part], t_ref.at[part], sem.at[2 * c + 1]),
            )
        )
    for w_copy, t_copy in copies:
        w_copy.start()
        t_copy.start()
    small[2].start()
    small[3].start()
    small[0].wait()
    small[1].wait()

    mask = eye(rank, rank)
    mask2 = eye(rank, 2 * rank)
    lane = lax.broadcasted_iota(jnp.int32, (leaves, 2 * rank), 1)
    charge = q[...]
    coords = [pts[c] for c in range(3)]
    twice = [jnp.where(lane < rank, x, pltpu.roll(x, rank, 1)) for x in coords]
    other = pltpu.roll(charge, rank, 1)
    for i in range(leaves):
        for r, x in ((0, coords[0]), (1, coords[1]), (2, coords[2]), (3, charge)):
            pack[i, r : r + 1, :] = x[i : i + 1, :]
        for r in range(3):
            pack[i, 5 + r : 6 + r, :] = twice[r][i : i + 1, :]

    total = jnp.zeros((rank, rank), jnp.float32)
    for c in range(CHUNKS):
        copies[c][0].wait()
        copies[c][1].wait()
        for i in range(c * step, (c + 1) * step):
            own = jnp.where(mask, charge[i : i + 1, :rank], 0.0)
            col = jnp.sum(w_ref[i] * other[i : i + 1, :rank] + own, axis=1, keepdims=True)
            total = total + t_ref[i] * col
            pack[i, 4:5, :] = to_row(col, mask2)
    lo[...] = pack[0:HALO]
    hi[...] = pack[leaves - HALO : leaves]
    small[2].wait()
    small[3].wait()

    rows = [jnp.sum(total, axis=0, keepdims=True)]
    for k in range(0, lay.levels - 1, 2):
        col = jnp.sum(jnp.transpose(e_ref[k]) * rows[k], axis=1, keepdims=True)
        rows.append(to_row(col, mask))
        if k + 2 < lay.levels:
            rows.append(jnp.sum(e_ref[k + 1] * col, axis=0, keepdims=True))

    head = [side(rows[k], p_ref[3 * k]) for k in range(lay.levels)]
    tail = [side(p_ref[3 * k + 1], p_ref[3 * k + 2]) for k in range(lay.levels)]
    sums = [side(rows[pair[0]], rows[pair[-1]]) for pair in lay.pairs]
    for k in range(lay.levels):
        msg[2 * k] = head[k]
        msg[2 * k + 1] = tail[k]
    a, _ = lay.place()
    for diff in range(lay.na):
        base = (a ^ diff) * lay.rows_a
        k = lay.level_a(diff)
        for r, row in enumerate([head[k], tail[k]] + sums):
            send[base + r] = row


def gathered_a(lay, recv, a):
    near, every = [], []
    for j in range(len(lay.pairs)):
        rows = [recv[(a ^ diff) * lay.rows_a + 2 + j] for diff in range(lay.na)]
        part = sum(rows[1 : lay.nz], rows[0])
        near.append(part)
        every.append(sum(rows[lay.nz + 1 :], rows[lay.nz]) + part)
    core = [recv[(a ^ diff) * lay.rows_a] for diff in range(lay.nz, lay.na)]
    return near, every, sum(core[1:], core[0])


def mid_kernel(lay, recv, msg, send):
    rank = msg.shape[2] // 2
    a, b = lay.place()
    near, every, core = gathered_a(lay, recv, a)
    lane = lax.broadcasted_iota(jnp.int32, (1, 2 * rank), 1)
    head = {}
    for j, pair in enumerate(lay.pairs):
        for at, k in enumerate(pair):
            row = near[j] if k < lay.core else every[j]
            if at:
                row = pltpu.roll(row, rank, 1)
            head[k] = jnp.where(lane < rank, row, msg[2 * k])
    tail = {k: msg[2 * k + 1] for k in head}
    for diff in range(lay.nb):
        base = (b ^ diff) * lay.rows_b
        k = lay.level_b(diff)
        send[base] = head[k]
        send[base + 1] = tail[k]
        send[base + 2] = core


def near_kernel(near_list, near_count, far_list, pack, lo, hi, after, near_out, far_out, win, tgt, acc):
    del after
    leaves, lanes = pack.shape[0], pack.shape[2]
    rank = lanes // 2
    tiles = lanes // 8
    far_tiles = rank // 8
    win[0:HALO] = lo[...]
    win[HALO : HALO + leaves] = pack[...]
    win[HALO + leaves :] = hi[...]

    def spread(i, carry):
        cols = jnp.transpose(pack[i])
        for c in range(3):
            tgt[i, c] = jnp.broadcast_to(cols[:, c : c + 1], (lanes, lanes))
        return carry

    lax.fori_loop(0, leaves, spread, 0, unroll=4)

    def kernel_tile(i, t, xs):
        at = pl.ds(8 * t, 8)
        d0 = tgt[i, 0, at, :] - xs[0]
        d1 = tgt[i, 1, at, :] - xs[1]
        d2 = tgt[i, 2, at, :] - xs[2]
        return lax.rsqrt((d0 * d0 + d1 * d1 + d2 * d2) + SOFTENING)

    lane = lax.broadcasted_iota(jnp.int32, (8, lanes), 1)

    def leaf(i, carry):
        def slot(m, sums):
            j = near_list[m, i]
            xs = [jnp.broadcast_to(win[j, pl.ds(c, 1), :], (8, lanes)) for c in range(4)]
            return tuple(sums[t] + kernel_tile(i, t, xs) * xs[3] for t in range(tiles))

        zero = tuple(jnp.zeros((8, lanes), jnp.float32) for _ in range(tiles))
        sums = lax.fori_loop(0, near_count[i], slot, zero)
        for t in range(tiles):
            acc[i, 8 * t : 8 * t + 8, :] = sums[t]

        far = [jnp.zeros((8, lanes), jnp.float32) for _ in range(far_tiles)]
        for m in range(0, far_list.shape[0], 2):
            both = jnp.where(lane < rank, win[far_list[m, i]], win[far_list[m + 1, i]])
            xs = [jnp.broadcast_to(both[r : r + 1, :], (8, lanes)) for r in (5, 6, 7, 4)]
            for t in range(far_tiles):
                far[t] = far[t] + kernel_tile(i, t, xs) * xs[3]
        for t in range(far_tiles):
            fold = far[t] + pltpu.roll(far[t], rank, 1)
            far_out[i, 8 * t : 8 * t + 8, :] = fold[:, :rank]
        return carry

    lax.fori_loop(0, leaves, leaf, 0)

    def reduce(i, carry):
        near_out[i] = jnp.sum(jnp.transpose(acc[i]), axis=0, keepdims=True)
        return carry

    lax.fori_loop(0, leaves, reduce, 0, unroll=4)


def post_kernel(
    lay, recv_a, recv_b, p_ref, e_ref, near, far, w_hbm, t_hbm, out, w_ref, t_ref, p_s, row_s, up_s, sem
):
    leaves, rank = w_ref.shape[0], w_ref.shape[1]
    t_copy = pltpu.make_async_copy(t_hbm, t_ref, sem.at[0])
    w_copy = pltpu.make_async_copy(w_hbm, w_ref, sem.at[1])
    t_copy.start()
    w_copy.start()
    mask = eye(rank, rank)
    a, b = lay.place()
    got_a = lambda diff, r: recv_a[(a ^ diff) * lay.rows_a + r]
    got_b = lambda diff, r: recv_b[(b ^ diff) * lay.rows_b + r]
    for k in range(3 * lay.levels):
        p_s[k : k + 1, :] = p_ref[k]
    own = jnp.transpose(p_s[...])

    weight, first = {}, {}
    for diff in range(1, lay.na):
        k = lay.level_a(diff)
        row = got_a(diff, 0)
        weight[k] = weight[k] + row if k in weight else row
        if k not in first:
            first[k] = (row, got_a(diff, 1))
    for diff in range(1, lay.nb):
        k = lay.level_b(diff)
        row = got_b(diff, 0)
        weight[k] = weight[k] + row if k in weight else row
        if k not in first:
            first[k] = (row, got_b(diff, 1))
        if diff < lay.ny:
            weight[lay.core] = weight[lay.core] + got_b(diff, 2)

    coupling = []
    for k in range(lay.levels):
        top, bottom = first[k]
        xs = [top[:, rank:], bottom[:, :rank], bottom[:, rank:]]
        squares = 0.0
        for c in range(3):
            d = own[:, 3 * k + c : 3 * k + c + 1] - xs[c]
            squares = squares + d * d
        coupling.append(
            jnp.sum(lax.rsqrt(squares + SOFTENING) * weight[k][:, :rank], axis=1, keepdims=True)
        )

    value, is_col = coupling[-1], True
    for k in range(lay.levels - 2, -1, -1):
        if is_col:
            value = jnp.sum(jnp.transpose(e_ref[k]) * value, axis=0, keepdims=True) + to_row(coupling[k], mask)
        else:
            value = jnp.sum(e_ref[k] * value, axis=1, keepdims=True) + coupling[k]
        is_col = not is_col
    row = to_row(value, mask) if is_col else value

    t_copy.wait()
    w_copy.wait()
    for i in range(leaves):
        col = jnp.sum(t_ref[i] * row + far[i], axis=1, keepdims=True)
        row_s[i : i + 1, :] = to_row(col, mask)
        up_s[i : i + 1, :] = jnp.sum(w_ref[i] * col, axis=0, keepdims=True)
    for i in range(leaves):
        out[i : i + 1, :] = near[i]
    out[...] = out[...] + side(row_s[...], up_s[...])


def in_vmem(x):
    return x if INTERPRET else pltpu.with_memory_space_constraint(x, pltpu.VMEM)


def in_hbm(x):
    return x if INTERPRET else pltpu.with_memory_space_constraint(x, pltpu.HBM)


def made(shape):
    return jax.ShapeDtypeStruct(shape, jnp.float32) if INTERPRET else pltpu.VMEM(shape, jnp.float32)


def call(body, in_specs, outs, scratch, flops=0):
    kwargs = {"interpret": True} if INTERPRET else {}
    return pl.pallas_call(
        body,
        in_specs=in_specs,
        out_specs=tuple(pl.BlockSpec(memory_space=pltpu.VMEM) for _ in outs),
        out_shape=tuple(outs),
        scratch_shapes=scratch,
        compiler_params=pltpu.CompilerParams(vmem_limit_bytes=32 << 20),
        cost_estimate=pl.CostEstimate(flops=flops, transcendentals=0, bytes_accessed=1 << 16) if flops else None,
        **kwargs,
    )


VM = pl.BlockSpec(memory_space=pltpu.VMEM)
SM = pl.BlockSpec(memory_space=pltpu.SMEM)
HB = pl.BlockSpec(memory_space=pl.ANY if INTERPRET else pltpu.HBM)


def on_device(
    lay,
    points,
    charges,
    interpolant,
    leaf_transfer,
    node_transfer,
    node_points,
    near_list,
    near_count,
    far_list,
):
    leaves, rank = interpolant.shape[0], interpolant.shape[1]
    lanes = points.shape[2]
    levels = lay.levels
    pts = jnp.transpose(points, (1, 0, 2))
    transfers = node_transfer[0]
    centres = jnp.transpose(node_points, (1, 2, 0, 3)).reshape(3 * levels, 1, rank)
    vec = lambda n: made((n, 1, lanes))
    square = made((leaves, rank, rank))

    pack, lo, hi, send, msg, e_ref, p_ref = call(
        lambda *refs: pre_kernel(lay, *refs),
        [HB] * 6,
        [
            made((leaves, 8, lanes)),
            made((HALO, 8, lanes)),
            made((HALO, 8, lanes)),
            vec(lay.na * lay.rows_a),
            vec(2 * levels),
            made((levels, rank, rank)),
            made((3 * levels, 1, rank)),
        ],
        [
            pltpu.VMEM((3, leaves, lanes), jnp.float32),
            pltpu.VMEM((leaves, lanes), jnp.float32),
            pltpu.VMEM((leaves, rank, rank), jnp.float32),
            pltpu.VMEM((leaves, rank, rank), jnp.float32),
            pltpu.SemaphoreType.DMA((2 * CHUNKS + 4,)),
        ],
    )(*(in_hbm(x) for x in (pts, charges, centres, transfers, interpolant, leaf_transfer)))

    recv_a = lax.all_to_all(send, AXES, 0, 0, axis_index_groups=lay.groups_a(), tiled=True)
    count = lay.na * lay.nb
    up = [(i, i + 1) for i in range(count - 1)]
    low = lax.ppermute(hi, AXES, up)
    high = lax.ppermute(lo, AXES, [(b, a) for a, b in up])

    (send_b,) = call(
        lambda *refs: mid_kernel(lay, *refs), [VM, VM], [vec(lay.nb * lay.rows_b)], []
    )(in_vmem(recv_a), in_vmem(msg))
    recv_b = lax.all_to_all(send_b, AXES, 0, 0, axis_index_groups=lay.groups_b(), tiled=True)

    near, far = call(
        near_kernel,
        [SM, SM, SM, VM, VM, VM, VM],
        [vec(leaves), square],
        [
            pltpu.VMEM((leaves + 2 * HALO, 8, lanes), jnp.float32),
            pltpu.VMEM((leaves, 3, lanes, lanes), jnp.float32),
            pltpu.VMEM((leaves, lanes, lanes), jnp.float32),
        ],
        flops=200_000_000,
    )(near_list.T, near_count, far_list.T, in_vmem(pack), in_vmem(low), in_vmem(high), in_vmem(send_b))

    (out,) = call(
        lambda *refs: post_kernel(lay, *refs),
        [VM] * 6 + [HB] * 2,
        [jax.ShapeDtypeStruct((leaves, lanes), jnp.float32)],
        [
            pltpu.VMEM((leaves, rank, rank), jnp.float32),
            pltpu.VMEM((leaves, rank, rank), jnp.float32),
            pltpu.VMEM((-(-3 * levels // 8) * 8, rank), jnp.float32),
            pltpu.VMEM((leaves, rank), jnp.float32),
            pltpu.VMEM((leaves, rank), jnp.float32),
            pltpu.SemaphoreType.DMA((2,)),
        ],
    )(*(in_vmem(x) for x in (recv_a, recv_b, p_ref, e_ref, near, far)), in_hbm(interpolant), in_hbm(leaf_transfer))
    return out


def solution(mesh):
    lay = Layout(*(mesh.shape[name] for name in AXES))
    split = lambda rest: P(AXES, *([None] * rest))

    def body(*args):
        return on_device(lay, *args)

    return jax.shard_map(
        body,
        mesh=mesh,
        in_specs=(split(2), split(1), split(2), split(2), split(3), split(3), split(1), split(0), split(1)),
        out_specs=split(1),
        check_vma=False,
    )
```

```python
import jax
import jax.numpy as jnp
from jax import lax
from jax.experimental import pallas as pl
from jax.experimental.pallas import tpu as pltpu
from jax.sharding import PartitionSpec as P


HALO = 8
SOFTENING = 0.0625
AXES = ("gx", "gy", "gz")
INTERPRET = False
CHUNKS = 4
UNROLL = 4
FINISH = 4


class Layout:
    def __init__(self, nx, ny, nz):
        self.nx, self.ny, self.nz = nx, ny, nz
        self.bx, self.by, self.bz = (n.bit_length() - 1 for n in (nx, ny, nz))
        self.levels = self.bx + self.by + self.bz
        self.core = self.bz + self.by
        self.na = 2 * nz
        self.nb = (nx // 2) * ny
        self.low = list(range(self.bz, self.core))
        self.high = list(range(self.core + 1, self.levels))
        both = self.low + self.high
        self.pairs = [both[i : i + 2] for i in range(0, len(both), 2)]
        self.rows_a = 2 + len(self.pairs)
        self.rows_b = 3

    def device(self, a, b):
        gz, core = a % self.nz, a // self.nz
        gy, up = b % self.ny, b // self.ny
        return ((up * 2 + core) * self.ny + gy) * self.nz + gz

    def groups_a(self):
        return [[self.device(a, b) for a in range(self.na)] for b in range(self.nb)]

    def groups_b(self):
        return [[self.device(a, b) for b in range(self.nb)] for a in range(self.na)]

    def level_a(self, diff):
        if diff == 0:
            return 0
        return self.core if diff >= self.nz else diff.bit_length() - 1

    def level_b(self, diff):
        high, low = diff // self.ny, diff % self.ny
        if high:
            return self.core + high.bit_length()
        return self.bz + low.bit_length() - 1 if low else self.bz

    def place(self):
        gx, gy, gz = (lax.axis_index(name) for name in AXES)
        return (gx % 2) * self.nz + gz, (gx // 2) * self.ny + gy


def eye(rows, lanes):
    r = lax.broadcasted_iota(jnp.int32, (rows, lanes), 0)
    c = lax.broadcasted_iota(jnp.int32, (rows, lanes), 1)
    return r == c % rows


def to_row(col, mask):
    return jnp.sum(jnp.where(mask, col, 0.0), axis=0, keepdims=True)


def side(left, right):
    return jnp.concatenate([left, right], axis=1)


def pre_kernel(
    lay, pts_hbm, q_hbm, p_hbm, e_hbm, w_hbm, t_hbm, l1_hbm, l2_hbm, l3_hbm,
    pack, lo, hi, send, msg, e_ref, p_ref, l1, l2, l3, pts, q, w_ref, t_ref, sem,
):
    leaves, rank = w_ref.shape[0], w_ref.shape[1]
    step = leaves // CHUNKS
    small = [
        pltpu.make_async_copy(src, dst, sem.at[2 * CHUNKS + n])
        for n, (src, dst) in enumerate((
            (q_hbm, q),
            (pts_hbm, pts),
            (e_hbm, e_ref),
            (p_hbm, p_ref),
            (l1_hbm, l1),
            (l2_hbm, l2),
            (l3_hbm, l3),
        )
        )
    ]
    small[0].start()
    small[1].start()
    copies = []
    for c in range(CHUNKS):
        part = pl.ds(c * step, step)
        copies.append(
            (
                pltpu.make_async_copy(w_hbm.at[part], w_ref.at[part], sem.at[2 * c]),
                pltpu.make_async_copy(t_hbm.at[part], t_ref.at[part], sem.at[2 * c + 1]),
            )
        )
    for w_copy, t_copy in copies:
        w_copy.start()
        t_copy.start()
    for copy in small[2:]:
        copy.start()
    small[0].wait()
    small[1].wait()

    mask = eye(rank, rank)
    mask2 = eye(rank, 2 * rank)
    lane = lax.broadcasted_iota(jnp.int32, (leaves, 2 * rank), 1)
    charge = q[...]
    coords = [pts[c] for c in range(3)]
    twice = [jnp.where(lane < rank, x, pltpu.roll(x, rank, 1)) for x in coords]
    other = pltpu.roll(charge, rank, 1)
    for i in range(leaves):
        for r, x in ((0, coords[0]), (1, coords[1]), (2, coords[2]), (3, charge)):
            pack[i, r : r + 1, :] = x[i : i + 1, :]
        for r in range(3):
            pack[i, 5 + r : 6 + r, :] = twice[r][i : i + 1, :]

    total = jnp.zeros((rank, rank), jnp.float32)
    for c in range(CHUNKS):
        copies[c][0].wait()
        copies[c][1].wait()
        for i in range(c * step, (c + 1) * step):
            own = jnp.where(mask, charge[i : i + 1, :rank], 0.0)
            col = jnp.sum(w_ref[i] * other[i : i + 1, :rank] + own, axis=1, keepdims=True)
            total = total + t_ref[i] * col
            pack[i, 4:5, :] = to_row(col, mask2)
    lo[...] = pack[0:HALO]
    hi[...] = pack[leaves - HALO : leaves]
    for copy in small[2:]:
        copy.wait()

    rows = [jnp.sum(total, axis=0, keepdims=True)]
    for k in range(0, lay.levels - 1, 2):
        col = jnp.sum(jnp.transpose(e_ref[k]) * rows[k], axis=1, keepdims=True)
        rows.append(to_row(col, mask))
        if k + 2 < lay.levels:
            rows.append(jnp.sum(e_ref[k + 1] * col, axis=0, keepdims=True))

    head = [side(rows[k], p_ref[3 * k]) for k in range(lay.levels)]
    tail = [side(p_ref[3 * k + 1], p_ref[3 * k + 2]) for k in range(lay.levels)]
    sums = [side(rows[pair[0]], rows[pair[-1]]) for pair in lay.pairs]
    for k in range(lay.levels):
        msg[2 * k] = head[k]
        msg[2 * k + 1] = tail[k]
    a, _ = lay.place()
    for diff in range(lay.na):
        base = (a ^ diff) * lay.rows_a
        k = lay.level_a(diff)
        for r, row in enumerate([head[k], tail[k]] + sums):
            send[base + r] = row


def gathered_a(lay, recv, a):
    near, every = [], []
    for j in range(len(lay.pairs)):
        rows = [recv[(a ^ diff) * lay.rows_a + 2 + j] for diff in range(lay.na)]
        part = sum(rows[1 : lay.nz], rows[0])
        near.append(part)
        every.append(sum(rows[lay.nz + 1 :], rows[lay.nz]) + part)
    core = [recv[(a ^ diff) * lay.rows_a] for diff in range(lay.nz, lay.na)]
    return near, every, sum(core[1:], core[0])


def mid_kernel(lay, recv, msg, send, token):
    rank = msg.shape[2] // 2
    a, b = lay.place()
    near, every, core = gathered_a(lay, recv, a)
    lane = lax.broadcasted_iota(jnp.int32, (1, 2 * rank), 1)
    head = {}
    for j, pair in enumerate(lay.pairs):
        for at, k in enumerate(pair):
            row = near[j] if k < lay.core else every[j]
            if at:
                row = pltpu.roll(row, rank, 1)
            head[k] = jnp.where(lane < rank, row, msg[2 * k])
    tail = {k: msg[2 * k + 1] for k in head}
    for diff in range(lay.nb):
        base = (b ^ diff) * lay.rows_b
        k = lay.level_b(diff)
        send[base] = head[k]
        send[base + 1] = tail[k]
        send[base + 2] = core
    token[0] = core


def near_kernel(
    near_src, count_src, far_src, pack, lo, hi, after, t_hbm, w_hbm,
    near_out, far_out, w_out, near_list, near_count, far_list, win, tgt, acc, t_ref, sem,
):
    del after
    copies = [
        pltpu.make_async_copy(src, dst, sem.at[n])
        for n, (src, dst) in enumerate(
            (
                (near_src, near_list),
                (count_src, near_count),
                (far_src, far_list),
                (t_hbm, t_ref),
                (w_hbm, w_out),
            )
        )
    ]
    for copy in copies:
        copy.start()
    leaves, lanes = pack.shape[0], pack.shape[2]
    rank = lanes // 2
    tiles = lanes // 8
    far_tiles = rank // 8
    win[0:HALO] = lo[...]
    win[HALO : HALO + leaves] = pack[...]
    win[HALO + leaves :] = hi[...]

    pick = lax.broadcasted_iota(jnp.int32, (32, 3 * lanes), 0) % 8
    wide = lax.broadcasted_iota(jnp.int32, (32, 3 * lanes), 1) // lanes
    choose = jnp.where(pick == wide, 1.0, 0.0).astype(jnp.bfloat16)
    used = lax.broadcasted_iota(jnp.int32, (8, lanes), 0) < 3

    def spread(i):
        x = jnp.where(used, win[HALO + i], 0.0)
        high = x.astype(jnp.bfloat16).astype(jnp.float32)
        rest = x - high
        mid = rest.astype(jnp.bfloat16).astype(jnp.float32)
        parts = jnp.concatenate([high, mid, rest - mid, jnp.zeros_like(x)], axis=0)
        cols = jnp.transpose(parts).astype(jnp.bfloat16)
        out = jnp.dot(cols, choose, preferred_element_type=jnp.float32)
        return [out[:, c * lanes : (c + 1) * lanes] for c in range(3)]

    def keep(i, cols):
        for c in range(3):
            tgt[i, c] = cols[c]

    for i in range(UNROLL):
        keep(i, spread(i))
    for copy in copies[:3]:
        copy.wait()

    def weighted(i, t, xs):
        at = pl.ds(8 * t, 8)
        d0 = tgt[i, 0, at, :] - xs[0]
        d1 = tgt[i, 1, at, :] - xs[1]
        d2 = tgt[i, 2, at, :] - xs[2]
        return lax.rsqrt((d0 * d0 + d1 * d1 + d2 * d2) + SOFTENING) * xs[3]

    def rows(j, which):
        return [jnp.broadcast_to(win[j, pl.ds(r, 1), :], (8, lanes)) for r in which]

    lane = lax.broadcasted_iota(jnp.int32, (8, lanes), 1)

    def far_field(g, carry):
        ahead = [spread((g + 1) * UNROLL + u) for u in range(UNROLL)]
        for u in range(UNROLL):
            i = g * UNROLL + u
            both = []
            for m in range(0, far_list.shape[0], 2):
                block = jnp.where(lane < rank, win[far_list[m, i]], win[far_list[m + 1, i]])
                both.append([jnp.broadcast_to(block[r : r + 1, :], (8, lanes)) for r in (5, 6, 7, 4)])
            for t in range(far_tiles):
                far = weighted(i, t, both[0])
                for xs in both[1:]:
                    far = far + weighted(i, t, xs)
                far_out[i, pl.ds(8 * t, 8), :] = far + pltpu.roll(far, rank, 1)
        for u in range(UNROLL):
            i = (g + 1) * UNROLL + u
            keep(i, ahead[u])
        return carry

    lax.fori_loop(0, leaves // UNROLL, far_field, 0)

    def leaf(i, carry):
        count = near_count[i]
        for t in range(tiles):
            acc[i, pl.ds(8 * t, 8), :] = jnp.zeros((8, lanes), jnp.float32)

        def slots(n, inner):
            m = 2 * n + 1
            one = rows(near_list[m, i], range(4))
            then = jnp.minimum(m + 1, near_list.shape[0] - 1)
            two = rows(near_list[then, i], range(4))
            two[3] = two[3] * jnp.where(m + 1 < count, 1.0, 0.0)
            for t in range(tiles):
                at = pl.ds(8 * t, 8)
                acc[i, at, :] = acc[i, at, :] + (weighted(i, t, one) + weighted(i, t, two))
            return inner

        return lax.fori_loop(0, count // 2, slots, carry)

    lax.fori_loop(0, leaves, leaf, 0)
    copies[3].wait()

    def finish(i, carry):
        own = rows(near_list[0, i], range(4))
        sums = [acc[i, pl.ds(8 * t, 8), :] + weighted(i, t, own) for t in range(tiles)]
        whole = jnp.concatenate(sums, axis=0)
        near_out[i] = jnp.sum(jnp.transpose(whole), axis=0, keepdims=True)
        for t in range(far_tiles):
            at = pl.ds(8 * t, 8)
            tile = t_ref[i, at, :]
            far_out[i, at, :] = jnp.where(lane < rank, side(tile, tile), far_out[i, at, :])
        return carry

    lax.fori_loop(0, leaves, finish, 0, unroll=FINISH)
    copies[4].wait()


def post_kernel(lay, recv_a, recv_b, p_ref, e_ref, near, far, w_ref, out, p_s, row_s, up_s):
    leaves, rank = w_ref.shape[0], w_ref.shape[1]
    mask = eye(rank, rank)
    a, b = lay.place()
    got_a = lambda diff, r: recv_a[(a ^ diff) * lay.rows_a + r]
    got_b = lambda diff, r: recv_b[(b ^ diff) * lay.rows_b + r]
    for k in range(3 * lay.levels):
        p_s[k : k + 1, :] = p_ref[k]
    own = jnp.transpose(p_s[...])

    weight, first = {}, {}
    for diff in range(1, lay.na):
        k = lay.level_a(diff)
        row = got_a(diff, 0)
        weight[k] = weight[k] + row if k in weight else row
        if k not in first:
            first[k] = (row, got_a(diff, 1))
    for diff in range(1, lay.nb):
        k = lay.level_b(diff)
        row = got_b(diff, 0)
        weight[k] = weight[k] + row if k in weight else row
        if k not in first:
            first[k] = (row, got_b(diff, 1))
        if diff < lay.ny:
            weight[lay.core] = weight[lay.core] + got_b(diff, 2)

    coupling = []
    for k in range(lay.levels):
        top, bottom = first[k]
        xs = [top[:, rank:], bottom[:, :rank], bottom[:, rank:]]
        squares = 0.0
        for c in range(3):
            d = own[:, 3 * k + c : 3 * k + c + 1] - xs[c]
            squares = squares + d * d
        coupling.append(
            jnp.sum(lax.rsqrt(squares + SOFTENING) * weight[k][:, :rank], axis=1, keepdims=True)
        )

    value, is_col = coupling[-1], True
    for k in range(lay.levels - 2, -1, -1):
        if is_col:
            value = jnp.sum(jnp.transpose(e_ref[k]) * value, axis=0, keepdims=True) + to_row(coupling[k], mask)
        else:
            value = jnp.sum(e_ref[k] * value, axis=1, keepdims=True) + coupling[k]
        is_col = not is_col
    row = to_row(value, eye(rank, 2 * rank)) if is_col else side(value, value)
    lane = lax.broadcasted_iota(jnp.int32, (1, 2 * rank), 1)
    row = jnp.where(lane < rank, row, 1.0)

    for i in range(leaves):
        col = jnp.sum(far[i] * row, axis=1, keepdims=True)
        row_s[i : i + 1, :] = to_row(col, mask)
        up_s[i : i + 1, :] = jnp.sum(w_ref[i] * col, axis=0, keepdims=True)
    for i in range(leaves):
        out[i : i + 1, :] = near[i]
    out[...] = out[...] + side(row_s[...], up_s[...])


def in_vmem(x):
    return x if INTERPRET else pltpu.with_memory_space_constraint(x, pltpu.VMEM)


def in_hbm(x):
    return x if INTERPRET else pltpu.with_memory_space_constraint(x, pltpu.HBM)


def made(shape, dtype=jnp.float32):
    return jax.ShapeDtypeStruct(shape, dtype) if INTERPRET else pltpu.VMEM(shape, dtype)


def call(body, in_specs, outs, scratch, flops=0):
    kwargs = {"interpret": True} if INTERPRET else {}
    return pl.pallas_call(
        body,
        in_specs=in_specs,
        out_specs=tuple(pl.BlockSpec(memory_space=pltpu.VMEM) for _ in outs),
        out_shape=tuple(outs),
        scratch_shapes=scratch,
        compiler_params=pltpu.CompilerParams(vmem_limit_bytes=32 << 20),
        cost_estimate=pl.CostEstimate(flops=flops, transcendentals=0, bytes_accessed=1 << 16) if flops else None,
        **kwargs,
    )


VM = pl.BlockSpec(memory_space=pltpu.VMEM)
SM = pl.BlockSpec(memory_space=pltpu.SMEM)
HB = pl.BlockSpec(memory_space=pl.ANY if INTERPRET else pltpu.HBM)


def on_device(
    lay,
    points,
    charges,
    interpolant,
    leaf_transfer,
    node_transfer,
    node_points,
    near_list,
    near_count,
    far_list,
):
    leaves, rank = interpolant.shape[0], interpolant.shape[1]
    lanes = points.shape[2]
    levels = lay.levels
    pts = jnp.transpose(points, (1, 0, 2))
    transfers = node_transfer[0]
    centres = jnp.transpose(node_points, (1, 2, 0, 3)).reshape(3 * levels, 1, rank)
    tables = (near_list.T, near_count, far_list.T)
    vec = lambda n: made((n, 1, lanes))

    pack, lo, hi, send, msg, e_ref, p_ref, *lists = call(
        lambda *refs: pre_kernel(lay, *refs),
        [HB] * 9,
        [
            made((leaves, 8, lanes)),
            made((HALO, 8, lanes)),
            made((HALO, 8, lanes)),
            vec(lay.na * lay.rows_a),
            vec(2 * levels),
            made((levels, rank, rank)),
            made((3 * levels, 1, rank)),
            *(made(x.shape, jnp.int32) for x in tables),
        ],
        [
            pltpu.VMEM((3, leaves, lanes), jnp.float32),
            pltpu.VMEM((leaves, lanes), jnp.float32),
            pltpu.VMEM((leaves, rank, rank), jnp.float32),
            pltpu.VMEM((leaves, rank, rank), jnp.float32),
            pltpu.SemaphoreType.DMA((2 * CHUNKS + 7,)),
        ],
    )(*(in_hbm(x) for x in (pts, charges, centres, transfers, interpolant, leaf_transfer, *tables)))

    recv_a = lax.all_to_all(send, AXES, 0, 0, axis_index_groups=lay.groups_a(), tiled=True)
    count = lay.na * lay.nb
    up = [(i, i + 1) for i in range(count - 1)]
    low = lax.ppermute(hi, AXES, up)
    high = lax.ppermute(lo, AXES, [(b, a) for a, b in up])

    send_b, token = call(
        lambda *refs: mid_kernel(lay, *refs), [VM, VM], [vec(lay.nb * lay.rows_b), vec(1)], []
    )(in_vmem(recv_a), in_vmem(msg))
    recv_b = lax.all_to_all(send_b, AXES, 0, 0, axis_index_groups=lay.groups_b(), tiled=True)

    near, far, w_ref = near_call(
        *lists, pack, low, high, token, leaf_transfer, interpolant
    )

    (out,) = call(
        lambda *refs: post_kernel(lay, *refs),
        [VM] * 7,
        [jax.ShapeDtypeStruct((leaves, lanes), jnp.float32)],
        [
            pltpu.VMEM((-(-3 * levels // 8) * 8, rank), jnp.float32),
            pltpu.VMEM((leaves, rank), jnp.float32),
            pltpu.VMEM((leaves, rank), jnp.float32),
        ],
    )(*(in_vmem(x) for x in (recv_a, recv_b, p_ref, e_ref, near, far, w_ref)))
    return out


def near_call(near_list, near_count, far_list, pack, low, high, token, leaf_transfer, interpolant):
    leaves, rank = interpolant.shape[0], interpolant.shape[1]
    lanes = pack.shape[2]
    return call(
        near_kernel,
        [VM] * 7 + [HB] * 2,
        [made((leaves, 1, lanes)), made((leaves, rank, lanes)), made((leaves, rank, rank))],
        [
            pltpu.SMEM(near_list.shape, jnp.int32),
            pltpu.SMEM(near_count.shape, jnp.int32),
            pltpu.SMEM(far_list.shape, jnp.int32),
            pltpu.VMEM((leaves + 2 * HALO, 8, lanes), jnp.float32),
            pltpu.VMEM((leaves + UNROLL, 3, lanes, lanes), jnp.float32),
            pltpu.VMEM((leaves, lanes, lanes), jnp.float32),
            pltpu.VMEM((leaves, rank, rank), jnp.float32),
            pltpu.SemaphoreType.DMA((5,)),
        ],
        flops=200_000_000,
    )(
        *(in_vmem(x) for x in (near_list, near_count, far_list, pack, low, high, token)),
        *(in_hbm(x) for x in (leaf_transfer, interpolant)),
    )


def solution(mesh):
    lay = Layout(*(mesh.shape[name] for name in AXES))
    split = lambda rest: P(AXES, *([None] * rest))

    def body(*args):
        return on_device(lay, *args)

    return jax.shard_map(
        body,
        mesh=mesh,
        in_specs=(split(2), split(1), split(2), split(2), split(3), split(3), split(1), split(0), split(1)),
        out_specs=split(1),
        check_vma=False,
    )
```

```python
import jax
import jax.numpy as jnp
from jax import lax
from jax.experimental import pallas as pl
from jax.experimental.pallas import tpu as pltpu
from jax.sharding import PartitionSpec as P


HALO = 8
SOFTENING = 0.0625
AXES = ("gx", "gy", "gz")
INTERPRET = False
CHUNKS = 4
UNROLL = 8
FINISH = 8


class Layout:
    def __init__(self, nx, ny, nz):
        self.nx, self.ny, self.nz = nx, ny, nz
        self.bx, self.by, self.bz = (n.bit_length() - 1 for n in (nx, ny, nz))
        self.levels = self.bx + self.by + self.bz
        self.core = self.bz + self.by
        self.na = 2 * nz
        self.nb = (nx // 2) * ny
        self.low = list(range(self.bz, self.core))
        self.high = list(range(self.core + 1, self.levels))
        both = self.low + self.high
        self.pairs = [both[i : i + 2] for i in range(0, len(both), 2)]
        self.rows_a = 2 + len(self.pairs)
        self.rows_b = 3
        self.couples = [(k, min(k + 1, self.levels - 1)) for k in range(0, self.levels, 2)]

    def device(self, a, b):
        gz, core = a % self.nz, a // self.nz
        gy, up = b % self.ny, b // self.ny
        return ((up * 2 + core) * self.ny + gy) * self.nz + gz

    def groups_a(self):
        return [[self.device(a, b) for a in range(self.na)] for b in range(self.nb)]

    def groups_b(self):
        return [[self.device(a, b) for b in range(self.nb)] for a in range(self.na)]

    def level_a(self, diff):
        if diff == 0:
            return 0
        return self.core if diff >= self.nz else diff.bit_length() - 1

    def level_b(self, diff):
        high, low = diff // self.ny, diff % self.ny
        if high:
            return self.core + high.bit_length()
        return self.bz + low.bit_length() - 1 if low else self.bz

    def place(self):
        gx, gy, gz = (lax.axis_index(name) for name in AXES)
        return (gx % 2) * self.nz + gz, (gx // 2) * self.ny + gy


def eye(rows, lanes):
    r = lax.broadcasted_iota(jnp.int32, (rows, lanes), 0)
    c = lax.broadcasted_iota(jnp.int32, (rows, lanes), 1)
    return r == c % rows


def to_row(col, mask):
    return jnp.sum(jnp.where(mask, col, 0.0), axis=0, keepdims=True)


def product(x, y):
    return jnp.dot(x, y, precision=lax.Precision.HIGHEST, preferred_element_type=jnp.float32)


def side(left, right):
    return jnp.concatenate([left, right], axis=1)


def pre_kernel(
    lay, pts_hbm, q_hbm, p_hbm, e_hbm, w_hbm, t_hbm, l1_hbm, l2_hbm, l3_hbm,
    pack, lo, hi, send, msg, f_ref, p_ref, l1, l2, l3, pts, q, w_ref, t_ref, e_ref, sem,
):
    leaves, rank = w_ref.shape[0], w_ref.shape[1]
    step = leaves // CHUNKS
    small = [
        pltpu.make_async_copy(src, dst, sem.at[2 * CHUNKS + n])
        for n, (src, dst) in enumerate((
            (q_hbm, q),
            (pts_hbm, pts),
            (e_hbm, e_ref),
            (p_hbm, p_ref),
            (l1_hbm, l1),
            (l2_hbm, l2),
            (l3_hbm, l3),
        )
        )
    ]
    for copy in small[:3]:
        copy.start()
    copies = []
    for c in range(CHUNKS):
        part = pl.ds(c * step, step)
        copies.append(
            (
                pltpu.make_async_copy(w_hbm.at[part], w_ref.at[part], sem.at[2 * c]),
                pltpu.make_async_copy(t_hbm.at[part], t_ref.at[part], sem.at[2 * c + 1]),
            )
        )
    for w_copy, t_copy in copies:
        w_copy.start()
        t_copy.start()
    for copy in small[3:]:
        copy.start()
    small[0].wait()
    small[1].wait()

    mask = eye(rank, rank)
    mask2 = eye(rank, 2 * rank)
    lane = lax.broadcasted_iota(jnp.int32, (leaves, 2 * rank), 1)
    charge = q[...]
    coords = [pts[c] for c in range(3)]
    twice = [jnp.where(lane < rank, x, pltpu.roll(x, rank, 1)) for x in coords]
    other = pltpu.roll(charge, rank, 1)
    for i in range(leaves):
        for r, x in ((0, coords[0]), (1, coords[1]), (2, coords[2]), (3, charge)):
            pack[i, r : r + 1, :] = x[i : i + 1, :]
        for r in range(3):
            pack[i, 5 + r : 6 + r, :] = twice[r][i : i + 1, :]

    assert lay.levels <= 2 * CHUNKS + 1
    total = jnp.zeros((rank, rank), jnp.float32)
    for c in range(CHUNKS):
        copies[c][0].wait()
        copies[c][1].wait()
        if c == 0:
            small[2].wait()
            f_ref[0] = e_ref[0]
            doubles = {k: product(e_ref[k], e_ref[k + 1]) for k in range(0, lay.levels - 2, 2)}
            if doubles:
                f_ref[1] = doubles[0]
        else:
            for k in (2 * c, 2 * c + 1):
                if k < lay.levels - 1:
                    f_ref[k] = product(f_ref[2 * c - 1], doubles[k - 1] if k % 2 else e_ref[k])
        for i in range(c * step, (c + 1) * step):
            own = jnp.where(mask, charge[i : i + 1, :rank], 0.0)
            col = jnp.sum(w_ref[i] * other[i : i + 1, :rank] + own, axis=1, keepdims=True)
            total = total + t_ref[i] * col
            pack[i, 4:5, :] = to_row(col, mask2)
    lo[...] = pack[0:HALO]
    hi[...] = pack[leaves - HALO : leaves]
    for copy in small[3:]:
        copy.wait()

    rows = [jnp.sum(total, axis=0, keepdims=True)]
    col = jnp.sum(jnp.where(mask, rows[0], 0.0), axis=1, keepdims=True)
    for k in range(1, lay.levels):
        rows.append(jnp.sum(f_ref[k - 1] * col, axis=0, keepdims=True))

    head = [side(rows[k], p_ref[3 * k]) for k in range(lay.levels)]
    tail = [side(p_ref[3 * k + 1], p_ref[3 * k + 2]) for k in range(lay.levels)]
    sums = [side(rows[pair[0]], rows[pair[-1]]) for pair in lay.pairs]
    for k in range(lay.levels):
        msg[2 * k] = head[k]
        msg[2 * k + 1] = tail[k]
    a, _ = lay.place()
    for diff in range(lay.na):
        base = (a ^ diff) * lay.rows_a
        k = lay.level_a(diff)
        for r, row in enumerate([head[k], tail[k]] + sums):
            send[base + r] = row


def gathered_a(lay, recv, a):
    near, every = [], []
    for j in range(len(lay.pairs)):
        rows = [recv[(a ^ diff) * lay.rows_a + 2 + j] for diff in range(lay.na)]
        part = sum(rows[1 : lay.nz], rows[0])
        near.append(part)
        every.append(sum(rows[lay.nz + 1 :], rows[lay.nz]) + part)
    core = [recv[(a ^ diff) * lay.rows_a] for diff in range(lay.nz, lay.na)]
    return near, every, sum(core[1:], core[0])


def mid_kernel(lay, recv, msg, send, token):
    rank = msg.shape[2] // 2
    a, b = lay.place()
    near, every, core = gathered_a(lay, recv, a)
    lane = lax.broadcasted_iota(jnp.int32, (1, 2 * rank), 1)
    head = {}
    for j, pair in enumerate(lay.pairs):
        for at, k in enumerate(pair):
            row = near[j] if k < lay.core else every[j]
            if at:
                row = pltpu.roll(row, rank, 1)
            head[k] = jnp.where(lane < rank, row, msg[2 * k])
    tail = {k: msg[2 * k + 1] for k in head}
    for diff in range(lay.nb):
        base = (b ^ diff) * lay.rows_b
        k = lay.level_b(diff)
        send[base] = head[k]
        send[base + 1] = tail[k]
        send[base + 2] = core
    token[0] = core


def near_kernel(
    lay, near_src, count_src, far_src, pack, lo, hi, after, p_ref, t_hbm, w_hbm,
    near_out, far_out, w_out, node_out, p_s, near_list, near_count, far_list, win, tgt, acc, t_ref, sem,
):
    del after
    copies = [
        pltpu.make_async_copy(src, dst, sem.at[n])
        for n, (src, dst) in enumerate(
            (
                (near_src, near_list),
                (count_src, near_count),
                (far_src, far_list),
                (t_hbm, t_ref),
                (w_hbm, w_out),
            )
        )
    ]
    for copy in copies:
        copy.start()
    leaves, lanes = pack.shape[0], pack.shape[2]
    rank = lanes // 2
    tiles = lanes // 8
    far_tiles = rank // 8
    win[0:HALO] = lo[...]
    win[HALO : HALO + leaves] = pack[...]
    win[HALO + leaves :] = hi[...]

    pick = lax.broadcasted_iota(jnp.int32, (32, 3 * lanes), 0) % 8
    wide = lax.broadcasted_iota(jnp.int32, (32, 3 * lanes), 1) // lanes
    choose = jnp.where(pick == wide, 1.0, 0.0).astype(jnp.bfloat16)
    used = lax.broadcasted_iota(jnp.int32, (8, lanes), 0) < 3

    def spread(i):
        x = jnp.where(used, win[HALO + i], 0.0)
        high = x.astype(jnp.bfloat16).astype(jnp.float32)
        rest = x - high
        mid = rest.astype(jnp.bfloat16).astype(jnp.float32)
        parts = jnp.concatenate([high, mid, rest - mid, jnp.zeros_like(x)], axis=0)
        out = lax.dot_general(
            parts.astype(jnp.bfloat16), choose, (((0,), (0,)), ((), ())), preferred_element_type=jnp.float32
        )
        return [out[:, c * lanes : (c + 1) * lanes] for c in range(3)]

    def keep(i, cols):
        for c in range(3):
            tgt[i, c] = cols[c]

    for k in range(3 * lay.levels):
        p_s[k : k + 1, :] = p_ref[k]
    own = jnp.transpose(p_s[...])
    half = lax.broadcasted_iota(jnp.int32, (rank, lanes), 1) < rank
    for n, (one, two) in enumerate(lay.couples):
        for c in range(3):
            left, right = own[:, 3 * one + c : 3 * one + c + 1], own[:, 3 * two + c : 3 * two + c + 1]
            node_out[3 * n + c] = jnp.where(half, left, right)
    for i in range(UNROLL):
        keep(i, spread(i))
    for copy in copies[:3]:
        copy.wait()

    def weighted(i, t, xs):
        at = pl.ds(8 * t, 8)
        d0 = tgt[i, 0, at, :] - xs[0]
        d1 = tgt[i, 1, at, :] - xs[1]
        d2 = tgt[i, 2, at, :] - xs[2]
        return lax.rsqrt((d0 * d0 + d1 * d1 + d2 * d2) + SOFTENING) * xs[3]

    def rows(j, which):
        return [jnp.broadcast_to(win[j, pl.ds(r, 1), :], (8, lanes)) for r in which]

    lane = lax.broadcasted_iota(jnp.int32, (8, lanes), 1)

    def far_field(g, carry):
        ahead = [spread((g + 1) * UNROLL + u) for u in range(UNROLL)]
        for u in range(UNROLL):
            i = g * UNROLL + u
            both = []
            for m in range(0, far_list.shape[0], 2):
                block = jnp.where(lane < rank, win[far_list[m, i]], win[far_list[m + 1, i]])
                both.append([jnp.broadcast_to(block[r : r + 1, :], (8, lanes)) for r in (5, 6, 7, 4)])
            for t in range(far_tiles):
                far = weighted(i, t, both[0])
                for xs in both[1:]:
                    far = far + weighted(i, t, xs)
                far_out[i, pl.ds(8 * t, 8), :] = far + pltpu.roll(far, rank, 1)
        for u in range(UNROLL):
            i = (g + 1) * UNROLL + u
            keep(i, ahead[u])
        return carry

    lax.fori_loop(0, leaves // UNROLL, far_field, 0)

    def leaf(i, carry):
        count = near_count[i]
        for t in range(tiles):
            acc[i, pl.ds(8 * t, 8), :] = jnp.zeros((8, lanes), jnp.float32)

        def slots(n, inner):
            m = 2 * n + 1
            one = rows(near_list[m, i], range(4))
            then = jnp.minimum(m + 1, near_list.shape[0] - 1)
            two = rows(near_list[then, i], range(4))
            two[3] = two[3] * jnp.where(m + 1 < count, 1.0, 0.0)
            for t in range(tiles):
                at = pl.ds(8 * t, 8)
                acc[i, at, :] = acc[i, at, :] + (weighted(i, t, one) + weighted(i, t, two))
            return inner

        return lax.fori_loop(0, count // 2, slots, carry)

    lax.fori_loop(0, leaves, leaf, 0)
    copies[3].wait()

    def finish(i, carry):
        own = rows(near_list[0, i], range(4))
        sums = [acc[i, pl.ds(8 * t, 8), :] + weighted(i, t, own) for t in range(tiles)]
        whole = jnp.concatenate(sums, axis=0)
        near_out[i] = jnp.sum(jnp.transpose(whole), axis=0, keepdims=True)
        for t in range(far_tiles):
            at = pl.ds(8 * t, 8)
            tile = t_ref[i, at, :]
            far_out[i, at, :] = jnp.where(lane < rank, side(tile, tile), far_out[i, at, :])
        return carry

    lax.fori_loop(0, leaves, finish, 0, unroll=FINISH)
    copies[4].wait()


def post_kernel(lay, recv_a, recv_b, f_ref, near, far, w_ref, node, out, row_s, up_s):
    leaves, rank = w_ref.shape[0], w_ref.shape[1]
    mask = eye(rank, rank)
    a, b = lay.place()
    got_a = lambda diff, r: recv_a[(a ^ diff) * lay.rows_a + r]
    got_b = lambda diff, r: recv_b[(b ^ diff) * lay.rows_b + r]

    weight, first = {}, {}
    for diff in range(1, lay.na):
        k = lay.level_a(diff)
        row = got_a(diff, 0)
        weight[k] = weight[k] + row if k in weight else row
        if k not in first:
            first[k] = (row, got_a(diff, 1))
    for diff in range(1, lay.nb):
        k = lay.level_b(diff)
        row = got_b(diff, 0)
        weight[k] = weight[k] + row if k in weight else row
        if k not in first:
            first[k] = (row, got_b(diff, 1))
        if diff < lay.ny:
            weight[lay.core] = weight[lay.core] + got_b(diff, 2)

    lane = lax.broadcasted_iota(jnp.int32, (1, 2 * rank), 1)
    turned = lambda x: pltpu.roll(x, rank, 1)
    value, carried = 0.0, 0.0
    for n, (one, two) in enumerate(lay.couples):
        (top, bottom), (top2, bottom2) = first[one], first[two]
        xs = [
            jnp.where(lane < rank, turned(top), top2),
            jnp.where(lane < rank, bottom, turned(bottom2)),
            jnp.where(lane < rank, turned(bottom), bottom2),
        ]
        amount = jnp.where(lane < rank, weight[one], turned(weight[two]))
        squares = 0.0
        for c in range(3):
            d = node[3 * n + c] - xs[c]
            squares = squares + d * d
        terms = lax.rsqrt(squares + SOFTENING) * amount
        for k in (one,) if one == two else (one, two):
            keep = lane < rank if k == one else lane >= rank
            col = jnp.sum(jnp.where(keep, terms, 0.0), axis=1, keepdims=True)
            if k:
                carried = carried + f_ref[k - 1] * to_row(col, mask)
            else:
                value = col
    value = value + jnp.sum(carried, axis=1, keepdims=True)
    row = jnp.where(lane < rank, to_row(value, eye(rank, 2 * rank)), 1.0)

    for i in range(leaves):
        col = jnp.sum(far[i] * row, axis=1, keepdims=True)
        row_s[i : i + 1, :] = to_row(col, mask)
        up_s[i : i + 1, :] = jnp.sum(w_ref[i] * col, axis=0, keepdims=True)
    for i in range(leaves):
        out[i : i + 1, :] = near[i]
    out[...] = out[...] + side(row_s[...], up_s[...])


def in_vmem(x):
    return x if INTERPRET else pltpu.with_memory_space_constraint(x, pltpu.VMEM)


def in_hbm(x):
    return x if INTERPRET else pltpu.with_memory_space_constraint(x, pltpu.HBM)


def made(shape, dtype=jnp.float32):
    return jax.ShapeDtypeStruct(shape, dtype) if INTERPRET else pltpu.VMEM(shape, dtype)


def call(body, in_specs, outs, scratch, flops=0):
    kwargs = {"interpret": True} if INTERPRET else {}
    return pl.pallas_call(
        body,
        in_specs=in_specs,
        out_specs=tuple(pl.BlockSpec(memory_space=pltpu.VMEM) for _ in outs),
        out_shape=tuple(outs),
        scratch_shapes=scratch,
        compiler_params=pltpu.CompilerParams(vmem_limit_bytes=32 << 20),
        cost_estimate=pl.CostEstimate(flops=flops, transcendentals=0, bytes_accessed=1 << 16) if flops else None,
        **kwargs,
    )


VM = pl.BlockSpec(memory_space=pltpu.VMEM)
SM = pl.BlockSpec(memory_space=pltpu.SMEM)
HB = pl.BlockSpec(memory_space=pl.ANY if INTERPRET else pltpu.HBM)


def POST_IN():
    return [VM] * 7


def POST_SCRATCH(leaves, rank):
    return [
        pltpu.VMEM((leaves, rank), jnp.float32),
        pltpu.VMEM((leaves, rank), jnp.float32),
    ]


def on_device(
    lay,
    points,
    charges,
    interpolant,
    leaf_transfer,
    node_transfer,
    node_points,
    near_list,
    near_count,
    far_list,
):
    leaves, rank = interpolant.shape[0], interpolant.shape[1]
    lanes = points.shape[2]
    levels = lay.levels
    pts = jnp.transpose(points, (1, 0, 2))
    transfers = node_transfer[0]
    centres = jnp.transpose(node_points, (1, 2, 0, 3)).reshape(3 * levels, 1, rank)
    tables = (near_list.T, near_count, far_list.T)
    vec = lambda n: made((n, 1, lanes))

    pack, lo, hi, send, msg, f_ref, p_ref, *lists = call_pre(
        lay, pts, charges, centres, transfers, interpolant, leaf_transfer, tables
    )

    recv_a = lax.all_to_all(send, AXES, 0, 0, axis_index_groups=lay.groups_a(), tiled=True)
    count = lay.na * lay.nb
    up = [(i, i + 1) for i in range(count - 1)]
    low = lax.ppermute(hi, AXES, up)
    high = lax.ppermute(lo, AXES, [(b, a) for a, b in up])

    send_b, token = call(
        lambda *refs: mid_kernel(lay, *refs), [VM, VM], [vec(lay.nb * lay.rows_b), vec(1)], []
    )(in_vmem(recv_a), in_vmem(msg))
    recv_b = lax.all_to_all(send_b, AXES, 0, 0, axis_index_groups=lay.groups_b(), tiled=True)

    near, far, w_ref, node = near_call(
        lay, *lists, pack, low, high, token, p_ref, leaf_transfer, interpolant
    )

    (out,) = call(
        lambda *refs: post_kernel(lay, *refs),
        POST_IN(),
        [jax.ShapeDtypeStruct((leaves, lanes), jnp.float32)],
        POST_SCRATCH(leaves, rank),
    )(*(in_vmem(x) for x in (recv_a, recv_b, f_ref, near, far, w_ref, node)))
    return out


def call_pre(lay, pts, charges, centres, transfers, interpolant, leaf_transfer, tables):
    leaves, rank = interpolant.shape[0], interpolant.shape[1]
    lanes = charges.shape[1]
    levels = lay.levels
    vec = lambda n: made((n, 1, lanes))
    return call(
        lambda *refs: pre_kernel(lay, *refs),
        [HB] * 9,
        [
            made((leaves, 8, lanes)),
            made((HALO, 8, lanes)),
            made((HALO, 8, lanes)),
            vec(lay.na * lay.rows_a),
            vec(2 * levels),
            made((levels - 1, rank, rank)),
            made((3 * levels, 1, rank)),
            *(made(x.shape, jnp.int32) for x in tables),
        ],
        [
            pltpu.VMEM((3, leaves, lanes), jnp.float32),
            pltpu.VMEM((leaves, lanes), jnp.float32),
            pltpu.VMEM((leaves, rank, rank), jnp.float32),
            pltpu.VMEM((leaves, rank, rank), jnp.float32),
            pltpu.VMEM((levels, rank, rank), jnp.float32),
            pltpu.SemaphoreType.DMA((2 * CHUNKS + 7,)),
        ],
    )(*(in_hbm(x) for x in (pts, charges, centres, transfers, interpolant, leaf_transfer, *tables)))


def near_call(lay, near_list, near_count, far_list, pack, low, high, token, p_ref, leaf_transfer, interpolant):
    leaves, rank = interpolant.shape[0], interpolant.shape[1]
    lanes = pack.shape[2]
    return call(
        lambda *refs: near_kernel(lay, *refs),
        [VM] * 8 + [HB] * 2,
        [
            made((leaves, 1, lanes)),
            made((leaves, rank, lanes)),
            made((leaves, rank, rank)),
            made((3 * len(lay.couples), rank, lanes)),
        ],
        [
            pltpu.VMEM((-(-3 * lay.levels // 8) * 8, rank), jnp.float32),
            pltpu.SMEM(near_list.shape, jnp.int32),
            pltpu.SMEM(near_count.shape, jnp.int32),
            pltpu.SMEM(far_list.shape, jnp.int32),
            pltpu.VMEM((leaves + 2 * HALO, 8, lanes), jnp.float32),
            pltpu.VMEM((leaves + UNROLL, 3, lanes, lanes), jnp.float32),
            pltpu.VMEM((leaves, lanes, lanes), jnp.float32),
            pltpu.VMEM((leaves, rank, rank), jnp.float32),
            pltpu.SemaphoreType.DMA((5,)),
        ],
        flops=200_000_000,
    )(
        *(in_vmem(x) for x in (near_list, near_count, far_list, pack, low, high, token, p_ref)),
        *(in_hbm(x) for x in (leaf_transfer, interpolant)),
    )


def solution(mesh):
    lay = Layout(*(mesh.shape[name] for name in AXES))
    split = lambda rest: P(AXES, *([None] * rest))

    def body(*args):
        return on_device(lay, *args)

    return jax.shard_map(
        body,
        mesh=mesh,
        in_specs=(split(2), split(1), split(2), split(2), split(3), split(3), split(1), split(0), split(1)),
        out_specs=split(1),
        check_vma=False,
    )
```

```python
import jax
import jax.numpy as jnp
from jax import lax
from jax.experimental import pallas as pl
from jax.experimental.pallas import tpu as pltpu
from jax.sharding import PartitionSpec as P


HALO = 8
SOFTENING = 0.0625
AXES = ("gx", "gy", "gz")
INTERPRET = False
CHUNKS = 4
UNROLL = 8
FINISH = 8


class Layout:
    def __init__(self, nx, ny, nz):
        self.nx, self.ny, self.nz = nx, ny, nz
        self.bx, self.by, self.bz = (n.bit_length() - 1 for n in (nx, ny, nz))
        self.levels = self.bx + self.by + self.bz
        self.core = self.bz + self.by
        self.na = 2 * nz
        self.nb = (nx // 2) * ny
        self.low = list(range(self.bz, self.core))
        self.high = list(range(self.core + 1, self.levels))
        both = self.low + self.high
        self.pairs = [both[i : i + 2] for i in range(0, len(both), 2)]
        self.rows_a = 2 + len(self.pairs)
        self.rows_b = 3
        self.couples = [(k, min(k + 1, self.levels - 1)) for k in range(0, self.levels, 2)]

    def device(self, a, b):
        gz, core = a % self.nz, a // self.nz
        gy, up = b % self.ny, b // self.ny
        return ((up * 2 + core) * self.ny + gy) * self.nz + gz

    def groups_a(self):
        return [[self.device(a, b) for a in range(self.na)] for b in range(self.nb)]

    def groups_b(self):
        return [[self.device(a, b) for b in range(self.nb)] for a in range(self.na)]

    def level_a(self, diff):
        if diff == 0:
            return 0
        return self.core if diff >= self.nz else diff.bit_length() - 1

    def level_b(self, diff):
        high, low = diff // self.ny, diff % self.ny
        if high:
            return self.core + high.bit_length()
        return self.bz + low.bit_length() - 1 if low else self.bz

    def place(self):
        gx, gy, gz = (lax.axis_index(name) for name in AXES)
        return (gx % 2) * self.nz + gz, (gx // 2) * self.ny + gy


def eye(rows, lanes):
    r = lax.broadcasted_iota(jnp.int32, (rows, lanes), 0)
    c = lax.broadcasted_iota(jnp.int32, (rows, lanes), 1)
    return r == c % rows


def to_row(col, mask):
    return jnp.sum(jnp.where(mask, col, 0.0), axis=0, keepdims=True)


def product(x, y):
    return jnp.dot(x, y, precision=lax.Precision.HIGHEST, preferred_element_type=jnp.float32)


def side(left, right):
    return jnp.concatenate([left, right], axis=1)


def pre_kernel(
    lay, pts_hbm, q_hbm, p_hbm, e_hbm, w_hbm, t_hbm, l1_hbm, l2_hbm, l3_hbm,
    pack, lo, hi, send, msg, f_ref, p_ref, l1, l2, l3, pts, q, w_ref, t_ref, e_ref, sem,
):
    leaves, rank = w_ref.shape[0], w_ref.shape[1]
    step = leaves // CHUNKS
    small = [
        pltpu.make_async_copy(src, dst, sem.at[2 * CHUNKS + n])
        for n, (src, dst) in enumerate((
            (q_hbm, q),
            (pts_hbm, pts),
            (e_hbm, e_ref),
            (p_hbm, p_ref),
            (l1_hbm, l1),
            (l2_hbm, l2),
            (l3_hbm, l3),
        )
        )
    ]
    for copy in small[:3]:
        copy.start()
    copies = []
    for c in range(CHUNKS):
        part = pl.ds(c * step, step)
        copies.append(
            (
                pltpu.make_async_copy(w_hbm.at[part], w_ref.at[part], sem.at[2 * c]),
                pltpu.make_async_copy(t_hbm.at[part], t_ref.at[part], sem.at[2 * c + 1]),
            )
        )
    for w_copy, t_copy in copies:
        w_copy.start()
        t_copy.start()
    for copy in small[3:]:
        copy.start()
    small[0].wait()
    small[1].wait()

    mask = eye(rank, rank)
    mask2 = eye(rank, 2 * rank)
    lane = lax.broadcasted_iota(jnp.int32, (leaves, 2 * rank), 1)
    charge = q[...]
    coords = [pts[c] for c in range(3)]
    twice = [jnp.where(lane < rank, x, pltpu.roll(x, rank, 1)) for x in coords]
    other = pltpu.roll(charge, rank, 1)
    for i in range(leaves):
        for r, x in ((0, coords[0]), (1, coords[1]), (2, coords[2]), (3, charge)):
            pack[i, r : r + 1, :] = x[i : i + 1, :]
        for r in range(3):
            pack[i, 5 + r : 6 + r, :] = twice[r][i : i + 1, :]

    assert lay.levels <= 2 * CHUNKS + 1
    total = jnp.zeros((rank, rank), jnp.float32)
    for c in range(CHUNKS):
        copies[c][0].wait()
        copies[c][1].wait()
        if c == 0:
            small[2].wait()
            f_ref[0] = e_ref[0]
            doubles = {k: product(e_ref[k], e_ref[k + 1]) for k in range(0, lay.levels - 2, 2)}
            if doubles:
                f_ref[1] = doubles[0]
        else:
            for k in (2 * c, 2 * c + 1):
                if k < lay.levels - 1:
                    f_ref[k] = product(f_ref[2 * c - 1], doubles[k - 1] if k % 2 else e_ref[k])
        for i in range(c * step, (c + 1) * step):
            own = jnp.where(mask, charge[i : i + 1, :rank], 0.0)
            col = jnp.sum(w_ref[i] * other[i : i + 1, :rank] + own, axis=1, keepdims=True)
            total = total + t_ref[i] * col
            pack[i, 4:5, :] = to_row(col, mask2)
    lo[...] = pack[0:HALO]
    hi[...] = pack[leaves - HALO : leaves]
    for copy in small[3:]:
        copy.wait()

    rows = [jnp.sum(total, axis=0, keepdims=True)]
    col = jnp.sum(jnp.where(mask, rows[0], 0.0), axis=1, keepdims=True)
    for k in range(1, lay.levels):
        rows.append(jnp.sum(f_ref[k - 1] * col, axis=0, keepdims=True))

    head = [side(rows[k], p_ref[3 * k]) for k in range(lay.levels)]
    tail = [side(p_ref[3 * k + 1], p_ref[3 * k + 2]) for k in range(lay.levels)]
    sums = [side(rows[pair[0]], rows[pair[-1]]) for pair in lay.pairs]
    for k in range(lay.levels):
        msg[2 * k] = head[k]
        msg[2 * k + 1] = tail[k]
    a, _ = lay.place()
    for diff in range(lay.na):
        base = (a ^ diff) * lay.rows_a
        k = lay.level_a(diff)
        for r, row in enumerate([head[k], tail[k]] + sums):
            send[base + r] = row


def gathered_a(lay, recv, a):
    near, every = [], []
    for j in range(len(lay.pairs)):
        rows = [recv[(a ^ diff) * lay.rows_a + 2 + j] for diff in range(lay.na)]
        part = sum(rows[1 : lay.nz], rows[0])
        near.append(part)
        every.append(sum(rows[lay.nz + 1 :], rows[lay.nz]) + part)
    core = [recv[(a ^ diff) * lay.rows_a] for diff in range(lay.nz, lay.na)]
    return near, every, sum(core[1:], core[0])


def mid_kernel(lay, recv, msg, send, token):
    rank = msg.shape[2] // 2
    a, b = lay.place()
    near, every, core = gathered_a(lay, recv, a)
    lane = lax.broadcasted_iota(jnp.int32, (1, 2 * rank), 1)
    head = {}
    for j, pair in enumerate(lay.pairs):
        for at, k in enumerate(pair):
            row = near[j] if k < lay.core else every[j]
            if at:
                row = pltpu.roll(row, rank, 1)
            head[k] = jnp.where(lane < rank, row, msg[2 * k])
    tail = {k: msg[2 * k + 1] for k in head}
    for diff in range(lay.nb):
        base = (b ^ diff) * lay.rows_b
        k = lay.level_b(diff)
        send[base] = head[k]
        send[base + 1] = tail[k]
        send[base + 2] = core
    token[0] = core


def near_kernel(lay, start, near_src, count_src, far_src, pack, halo, after, *refs):
    del after
    head = start == 0
    if head:
        p_ref, t_hbm, w_hbm, near_out, far_out, w_out, node_out, p_s = refs[:8]
        refs = refs[8:]
    else:
        t_hbm, near_out, far_out = refs[:3]
        refs = refs[3:]
    near_list, near_count, far_list, win, tgt, acc, t_ref, sem = refs
    leaves, lanes = near_out.shape[0], pack.shape[2]
    rank = lanes // 2
    tiles = lanes // 8
    far_tiles = rank // 8
    moves = [
        (near_src, near_list),
        (count_src, near_count),
        (far_src, far_list),
        (t_hbm.at[pl.ds(start, leaves)], t_ref),
    ]
    if head:
        moves.append((w_hbm, w_out))
    copies = [pltpu.make_async_copy(src, dst, sem.at[n]) for n, (src, dst) in enumerate(moves)]
    for copy in copies:
        copy.start()
    total = pack.shape[0]
    if head:
        win[0:HALO] = halo[...]
    else:
        win[HALO + total :] = halo[...]
    win[HALO : HALO + total] = pack[...]

    pick = lax.broadcasted_iota(jnp.int32, (32, 3 * lanes), 0) % 8
    wide = lax.broadcasted_iota(jnp.int32, (32, 3 * lanes), 1) // lanes
    choose = jnp.where(pick == wide, 1.0, 0.0).astype(jnp.bfloat16)
    used = lax.broadcasted_iota(jnp.int32, (8, lanes), 0) < 3

    def spread(i):
        x = jnp.where(used, win[HALO + start + i], 0.0)
        high = x.astype(jnp.bfloat16).astype(jnp.float32)
        rest = x - high
        mid = rest.astype(jnp.bfloat16).astype(jnp.float32)
        parts = jnp.concatenate([high, mid, rest - mid, jnp.zeros_like(x)], axis=0)
        out = lax.dot_general(
            parts.astype(jnp.bfloat16), choose, (((0,), (0,)), ((), ())), preferred_element_type=jnp.float32
        )
        return [out[:, c * lanes : (c + 1) * lanes] for c in range(3)]

    def keep(i, cols):
        for c in range(3):
            tgt[i, c] = cols[c]

    if head:
        for k in range(3 * lay.levels):
            p_s[k : k + 1, :] = p_ref[k]
        own = jnp.transpose(p_s[...])
        half = lax.broadcasted_iota(jnp.int32, (rank, lanes), 1) < rank
        for n, (one, two) in enumerate(lay.couples):
            for c in range(3):
                left, right = own[:, 3 * one + c : 3 * one + c + 1], own[:, 3 * two + c : 3 * two + c + 1]
                node_out[3 * n + c] = jnp.where(half, left, right)
    for i in range(UNROLL):
        keep(i, spread(i))
    for copy in copies[:3]:
        copy.wait()

    def weighted(i, t, xs):
        at = pl.ds(8 * t, 8)
        d0 = tgt[i, 0, at, :] - xs[0]
        d1 = tgt[i, 1, at, :] - xs[1]
        d2 = tgt[i, 2, at, :] - xs[2]
        return lax.rsqrt((d0 * d0 + d1 * d1 + d2 * d2) + SOFTENING) * xs[3]

    def rows(j, which):
        return [jnp.broadcast_to(win[j, pl.ds(r, 1), :], (8, lanes)) for r in which]

    lane = lax.broadcasted_iota(jnp.int32, (8, lanes), 1)

    def far_field(g, more):
        ahead = [spread((g + 1) * UNROLL + u) for u in range(UNROLL)] if more else []
        for u in range(UNROLL):
            i = g * UNROLL + u
            both = []
            for m in range(0, far_list.shape[0], 2):
                block = jnp.where(lane < rank, win[far_list[m, start + i]], win[far_list[m + 1, start + i]])
                both.append([jnp.broadcast_to(block[r : r + 1, :], (8, lanes)) for r in (5, 6, 7, 4)])
            for t in range(far_tiles):
                far = weighted(i, t, both[0])
                for xs in both[1:]:
                    far = far + weighted(i, t, xs)
                far_out[i, pl.ds(8 * t, 8), :] = far + pltpu.roll(far, rank, 1)
        for u, cols in enumerate(ahead):
            keep((g + 1) * UNROLL + u, cols)

    def far_step(g, carry):
        far_field(g, True)
        return carry

    groups = leaves // UNROLL
    lax.fori_loop(0, groups - 1, far_step, 0)
    far_field(groups - 1, False)

    def leaf(i, carry):
        count = near_count[start + i]
        for t in range(tiles):
            acc[i, pl.ds(8 * t, 8), :] = jnp.zeros((8, lanes), jnp.float32)

        def slots(n, inner):
            m = 2 * n + 1
            one = rows(near_list[m, start + i], range(4))
            then = jnp.minimum(m + 1, near_list.shape[0] - 1)
            two = rows(near_list[then, start + i], range(4))
            two[3] = two[3] * jnp.where(m + 1 < count, 1.0, 0.0)
            for t in range(tiles):
                at = pl.ds(8 * t, 8)
                acc[i, at, :] = acc[i, at, :] + (weighted(i, t, one) + weighted(i, t, two))
            return inner

        return lax.fori_loop(0, count // 2, slots, carry)

    lax.fori_loop(0, leaves, leaf, 0)
    copies[3].wait()

    def finish(i, carry):
        own = rows(near_list[0, start + i], range(4))
        sums = [acc[i, pl.ds(8 * t, 8), :] + weighted(i, t, own) for t in range(tiles)]
        whole = jnp.concatenate(sums, axis=0)
        near_out[i] = jnp.sum(jnp.transpose(whole), axis=0, keepdims=True)
        for t in range(far_tiles):
            at = pl.ds(8 * t, 8)
            tile = t_ref[i, at, :]
            far_out[i, at, :] = jnp.where(lane < rank, side(tile, tile), far_out[i, at, :])
        return carry

    lax.fori_loop(0, leaves, finish, 0, unroll=FINISH)
    for copy in copies[4:]:
        copy.wait()


def post_kernel(lay, recv_a, recv_b, f_ref, near, far, near2, far2, w_ref, node, out, row_s, up_s):
    leaves, rank = w_ref.shape[0], w_ref.shape[1]
    mask = eye(rank, rank)
    a, b = lay.place()
    got_a = lambda diff, r: recv_a[(a ^ diff) * lay.rows_a + r]
    got_b = lambda diff, r: recv_b[(b ^ diff) * lay.rows_b + r]

    weight, first = {}, {}
    for diff in range(1, lay.na):
        k = lay.level_a(diff)
        row = got_a(diff, 0)
        weight[k] = weight[k] + row if k in weight else row
        if k not in first:
            first[k] = (row, got_a(diff, 1))
    for diff in range(1, lay.nb):
        k = lay.level_b(diff)
        row = got_b(diff, 0)
        weight[k] = weight[k] + row if k in weight else row
        if k not in first:
            first[k] = (row, got_b(diff, 1))
        if diff < lay.ny:
            weight[lay.core] = weight[lay.core] + got_b(diff, 2)

    lane = lax.broadcasted_iota(jnp.int32, (1, 2 * rank), 1)
    turned = lambda x: pltpu.roll(x, rank, 1)
    value, carried = 0.0, 0.0
    for n, (one, two) in enumerate(lay.couples):
        (top, bottom), (top2, bottom2) = first[one], first[two]
        xs = [
            jnp.where(lane < rank, turned(top), top2),
            jnp.where(lane < rank, bottom, turned(bottom2)),
            jnp.where(lane < rank, turned(bottom), bottom2),
        ]
        amount = jnp.where(lane < rank, weight[one], turned(weight[two]))
        squares = 0.0
        for c in range(3):
            d = node[3 * n + c] - xs[c]
            squares = squares + d * d
        terms = lax.rsqrt(squares + SOFTENING) * amount
        for k in (one,) if one == two else (one, two):
            keep = lane < rank if k == one else lane >= rank
            col = jnp.sum(jnp.where(keep, terms, 0.0), axis=1, keepdims=True)
            if k:
                carried = carried + f_ref[k - 1] * to_row(col, mask)
            else:
                value = col
    value = value + jnp.sum(carried, axis=1, keepdims=True)
    row = jnp.where(lane < rank, to_row(value, eye(rank, 2 * rank)), 1.0)

    split = far.shape[0]
    for i in range(leaves):
        sums = far[i] if i < split else far2[i - split]
        col = jnp.sum(sums * row, axis=1, keepdims=True)
        row_s[i : i + 1, :] = to_row(col, mask)
        up_s[i : i + 1, :] = jnp.sum(w_ref[i] * col, axis=0, keepdims=True)
    for i in range(leaves):
        out[i : i + 1, :] = near[i] if i < split else near2[i - split]
    out[...] = out[...] + side(row_s[...], up_s[...])


def in_vmem(x):
    return x if INTERPRET else pltpu.with_memory_space_constraint(x, pltpu.VMEM)


def in_hbm(x):
    return x if INTERPRET else pltpu.with_memory_space_constraint(x, pltpu.HBM)


def made(shape, dtype=jnp.float32):
    return jax.ShapeDtypeStruct(shape, dtype) if INTERPRET else pltpu.VMEM(shape, dtype)


def call(body, in_specs, outs, scratch, flops=0):
    kwargs = {"interpret": True} if INTERPRET else {}
    return pl.pallas_call(
        body,
        in_specs=in_specs,
        out_specs=tuple(pl.BlockSpec(memory_space=pltpu.VMEM) for _ in outs),
        out_shape=tuple(outs),
        scratch_shapes=scratch,
        compiler_params=pltpu.CompilerParams(vmem_limit_bytes=32 << 20),
        cost_estimate=pl.CostEstimate(flops=flops, transcendentals=0, bytes_accessed=1 << 16) if flops else None,
        **kwargs,
    )


VM = pl.BlockSpec(memory_space=pltpu.VMEM)
SM = pl.BlockSpec(memory_space=pltpu.SMEM)
HB = pl.BlockSpec(memory_space=pl.ANY if INTERPRET else pltpu.HBM)


def POST_IN():
    return [VM] * 9


def POST_SCRATCH(leaves, rank):
    return [
        pltpu.VMEM((leaves, rank), jnp.float32),
        pltpu.VMEM((leaves, rank), jnp.float32),
    ]


def on_device(
    lay,
    points,
    charges,
    interpolant,
    leaf_transfer,
    node_transfer,
    node_points,
    near_list,
    near_count,
    far_list,
):
    leaves, rank = interpolant.shape[0], interpolant.shape[1]
    lanes = points.shape[2]
    levels = lay.levels
    pts = jnp.transpose(points, (1, 0, 2))
    transfers = node_transfer[0]
    centres = jnp.transpose(node_points, (1, 2, 0, 3)).reshape(3 * levels, 1, rank)
    tables = (near_list.T, near_count, far_list.T)
    vec = lambda n: made((n, 1, lanes))

    pack, lo, hi, send, msg, f_ref, p_ref, *lists = call_pre(
        lay, pts, charges, centres, transfers, interpolant, leaf_transfer, tables
    )

    recv_a = lax.all_to_all(send, AXES, 0, 0, axis_index_groups=lay.groups_a(), tiled=True)
    count = lay.na * lay.nb
    up = [(i, i + 1) for i in range(count - 1)]
    low = lax.ppermute(hi, AXES, up)
    high = lax.ppermute(lo, AXES, [(b, a) for a, b in up])

    send_b, token = call(
        lambda *refs: mid_kernel(lay, *refs), [VM, VM], [vec(lay.nb * lay.rows_b), vec(1)], []
    )(in_vmem(recv_a), in_vmem(msg))
    recv_b = lax.all_to_all(send_b, AXES, 0, 0, axis_index_groups=lay.groups_b(), tiled=True)

    split = leaves - HALO
    near, far, w_ref, node = near_call(
        lay, 0, split, lists, pack, low, token, p_ref, leaf_transfer, interpolant
    )
    near2, far2 = near_call(lay, split, HALO, lists, pack, high, near, p_ref, leaf_transfer, interpolant)

    (out,) = call(
        lambda *refs: post_kernel(lay, *refs),
        POST_IN(),
        [jax.ShapeDtypeStruct((leaves, lanes), jnp.float32)],
        POST_SCRATCH(leaves, rank),
    )(*(in_vmem(x) for x in (recv_a, recv_b, f_ref, near, far, near2, far2, w_ref, node)))
    return out


def call_pre(lay, pts, charges, centres, transfers, interpolant, leaf_transfer, tables):
    leaves, rank = interpolant.shape[0], interpolant.shape[1]
    lanes = charges.shape[1]
    levels = lay.levels
    vec = lambda n: made((n, 1, lanes))
    return call(
        lambda *refs: pre_kernel(lay, *refs),
        [HB] * 9,
        [
            made((leaves, 8, lanes)),
            made((HALO, 8, lanes)),
            made((HALO, 8, lanes)),
            vec(lay.na * lay.rows_a),
            vec(2 * levels),
            made((levels - 1, rank, rank)),
            made((3 * levels, 1, rank)),
            *(made(x.shape, jnp.int32) for x in tables),
        ],
        [
            pltpu.VMEM((3, leaves, lanes), jnp.float32),
            pltpu.VMEM((leaves, lanes), jnp.float32),
            pltpu.VMEM((leaves, rank, rank), jnp.float32),
            pltpu.VMEM((leaves, rank, rank), jnp.float32),
            pltpu.VMEM((levels, rank, rank), jnp.float32),
            pltpu.SemaphoreType.DMA((2 * CHUNKS + 7,)),
        ],
    )(*(in_hbm(x) for x in (pts, charges, centres, transfers, interpolant, leaf_transfer, *tables)))


def near_call(lay, start, leaves, lists, pack, halo, token, p_ref, leaf_transfer, interpolant):
    total, rank = interpolant.shape[0], interpolant.shape[1]
    lanes = pack.shape[2]
    head = start == 0
    outs = [made((leaves, 1, lanes)), made((leaves, rank, lanes))]
    extra = []
    if head:
        outs += [made((total, rank, rank)), made((3 * len(lay.couples), rank, lanes))]
        extra = [pltpu.VMEM((-(-3 * lay.levels // 8) * 8, rank), jnp.float32)]
    near_inputs = [*lists, pack, halo, token] + ([p_ref] if head else [])
    far_inputs = [leaf_transfer] + ([interpolant] if head else [])
    return call(
        lambda *refs: near_kernel(lay, start, *refs),
        [VM] * len(near_inputs) + [HB] * len(far_inputs),
        outs,
        [
            *extra,
            *(pltpu.SMEM(x.shape, jnp.int32) for x in lists),
            pltpu.VMEM((total + 2 * HALO, 8, lanes), jnp.float32),
            pltpu.VMEM((leaves, 3, lanes, lanes), jnp.float32),
            pltpu.VMEM((leaves, lanes, lanes), jnp.float32),
            pltpu.VMEM((leaves, rank, rank), jnp.float32),
            pltpu.SemaphoreType.DMA((5,)),
        ],
        flops=200_000_000,
    )(*(in_vmem(x) for x in near_inputs), *(in_hbm(x) for x in far_inputs))


def solution(mesh):
    lay = Layout(*(mesh.shape[name] for name in AXES))
    split = lambda rest: P(AXES, *([None] * rest))

    def body(*args):
        return on_device(lay, *args)

    return jax.shard_map(
        body,
        mesh=mesh,
        in_specs=(split(2), split(1), split(2), split(2), split(3), split(3), split(1), split(0), split(1)),
        out_specs=split(1),
        check_vma=False,
    )
```

```python
import jax
import jax.numpy as jnp
from jax import lax
from jax.experimental import pallas as pl
from jax.experimental.pallas import tpu as pltpu
from jax.sharding import PartitionSpec as P


HALO = 8
SOFTENING = 0.0625
AXES = ("gx", "gy", "gz")
INTERPRET = False
CHUNKS = 4
UNROLL = 8
FINISH = 8


class Layout:
    def __init__(self, nx, ny, nz):
        self.nx, self.ny, self.nz = nx, ny, nz
        self.bx, self.by, self.bz = (n.bit_length() - 1 for n in (nx, ny, nz))
        self.levels = self.bx + self.by + self.bz
        self.core = self.bz + self.by
        self.na = 2 * nz
        self.nb = (nx // 2) * ny
        self.low = list(range(self.bz, self.core))
        self.high = list(range(self.core + 1, self.levels))
        both = self.low + self.high
        self.pairs = [both[i : i + 2] for i in range(0, len(both), 2)]
        self.rows_a = 2 + len(self.pairs)
        self.rows_b = 3
        self.couples = [(k, min(k + 1, self.levels - 1)) for k in range(0, self.levels, 2)]

    def device(self, a, b):
        gz, core = a % self.nz, a // self.nz
        gy, up = b % self.ny, b // self.ny
        return ((up * 2 + core) * self.ny + gy) * self.nz + gz

    def groups_a(self):
        return [[self.device(a, b) for a in range(self.na)] for b in range(self.nb)]

    def groups_b(self):
        return [[self.device(a, b) for b in range(self.nb)] for a in range(self.na)]

    def level_a(self, diff):
        if diff == 0:
            return 0
        return self.core if diff >= self.nz else diff.bit_length() - 1

    def level_b(self, diff):
        high, low = diff // self.ny, diff % self.ny
        if high:
            return self.core + high.bit_length()
        return self.bz + low.bit_length() - 1 if low else self.bz

    def place(self):
        gx, gy, gz = (lax.axis_index(name) for name in AXES)
        return (gx % 2) * self.nz + gz, (gx // 2) * self.ny + gy


def eye(rows, lanes):
    r = lax.broadcasted_iota(jnp.int32, (rows, lanes), 0)
    c = lax.broadcasted_iota(jnp.int32, (rows, lanes), 1)
    return r == c % rows


def to_row(col, mask):
    return jnp.sum(jnp.where(mask, col, 0.0), axis=0, keepdims=True)


def product(x, y):
    return jnp.dot(x, y, precision=lax.Precision.HIGHEST, preferred_element_type=jnp.float32)


def side(left, right):
    return jnp.concatenate([left, right], axis=1)


def pre_kernel(
    lay, pts_hbm, q_hbm, p_hbm, e_hbm, w_hbm, t_hbm, l1_hbm, l2_hbm, l3_hbm,
    pack, lo, hi, send, msg, f_ref, p_ref, l1, l2, l3, pts, q, w_ref, t_ref, e_ref, sem,
):
    leaves, rank = w_ref.shape[0], w_ref.shape[1]
    step = leaves // CHUNKS
    small = [
        pltpu.make_async_copy(src, dst, sem.at[2 * CHUNKS + n])
        for n, (src, dst) in enumerate((
            (q_hbm, q),
            (pts_hbm, pts),
            (e_hbm, e_ref),
            (p_hbm, p_ref),
            (l1_hbm, l1),
            (l2_hbm, l2),
            (l3_hbm, l3),
        )
        )
    ]
    for copy in small[:3]:
        copy.start()
    copies = []
    for c in range(CHUNKS):
        part = pl.ds(c * step, step)
        copies.append(
            (
                pltpu.make_async_copy(w_hbm.at[part], w_ref.at[part], sem.at[2 * c]),
                pltpu.make_async_copy(t_hbm.at[part], t_ref.at[part], sem.at[2 * c + 1]),
            )
        )
    for w_copy, t_copy in copies:
        w_copy.start()
        t_copy.start()
    for copy in small[3:]:
        copy.start()
    small[0].wait()
    small[1].wait()

    mask = eye(rank, rank)
    mask2 = eye(rank, 2 * rank)
    lane = lax.broadcasted_iota(jnp.int32, (leaves, 2 * rank), 1)
    charge = q[...]
    coords = [pts[c] for c in range(3)]
    twice = [jnp.where(lane < rank, x, pltpu.roll(x, rank, 1)) for x in coords]
    other = pltpu.roll(charge, rank, 1)
    for i in range(leaves):
        for r, x in ((0, coords[0]), (1, coords[1]), (2, coords[2]), (3, charge)):
            pack[i, r : r + 1, :] = x[i : i + 1, :]
        for r in range(3):
            pack[i, 5 + r : 6 + r, :] = twice[r][i : i + 1, :]

    assert lay.levels <= 2 * CHUNKS + 1
    total = jnp.zeros((rank, rank), jnp.float32)
    for c in range(CHUNKS):
        copies[c][0].wait()
        copies[c][1].wait()
        if c == 0:
            small[2].wait()
            f_ref[0] = e_ref[0]
            doubles = {k: product(e_ref[k], e_ref[k + 1]) for k in range(0, lay.levels - 2, 2)}
            if doubles:
                f_ref[1] = doubles[0]
        else:
            for k in (2 * c, 2 * c + 1):
                if k < lay.levels - 1:
                    f_ref[k] = product(f_ref[2 * c - 1], doubles[k - 1] if k % 2 else e_ref[k])
        for i in range(c * step, (c + 1) * step):
            own = jnp.where(mask, charge[i : i + 1, :rank], 0.0)
            col = jnp.sum(w_ref[i] * other[i : i + 1, :rank] + own, axis=1, keepdims=True)
            total = total + t_ref[i] * col
            pack[i, 4:5, :] = to_row(col, mask2)
    lo[...] = pack[0:HALO]
    hi[...] = pack[leaves - HALO : leaves]
    for copy in small[3:]:
        copy.wait()

    rows = [jnp.sum(total, axis=0, keepdims=True)]
    col = jnp.sum(jnp.where(mask, rows[0], 0.0), axis=1, keepdims=True)
    for k in range(1, lay.levels):
        rows.append(jnp.sum(f_ref[k - 1] * col, axis=0, keepdims=True))

    head = [side(rows[k], p_ref[3 * k]) for k in range(lay.levels)]
    tail = [side(p_ref[3 * k + 1], p_ref[3 * k + 2]) for k in range(lay.levels)]
    sums = [side(rows[pair[0]], rows[pair[-1]]) for pair in lay.pairs]
    for k in range(lay.levels):
        msg[2 * k] = head[k]
        msg[2 * k + 1] = tail[k]
    a, _ = lay.place()
    for diff in range(lay.na):
        base = (a ^ diff) * lay.rows_a
        k = lay.level_a(diff)
        for r, row in enumerate([head[k], tail[k]] + sums):
            send[base + r] = row


def gathered_a(lay, recv, a):
    near, every = [], []
    for j in range(len(lay.pairs)):
        rows = [recv[(a ^ diff) * lay.rows_a + 2 + j] for diff in range(lay.na)]
        part = sum(rows[1 : lay.nz], rows[0])
        near.append(part)
        every.append(sum(rows[lay.nz + 1 :], rows[lay.nz]) + part)
    core = [recv[(a ^ diff) * lay.rows_a] for diff in range(lay.nz, lay.na)]
    return near, every, sum(core[1:], core[0])


def mid_kernel(lay, recv, msg, send, token):
    rank = msg.shape[2] // 2
    a, b = lay.place()
    near, every, core = gathered_a(lay, recv, a)
    lane = lax.broadcasted_iota(jnp.int32, (1, 2 * rank), 1)
    head = {}
    for j, pair in enumerate(lay.pairs):
        for at, k in enumerate(pair):
            row = near[j] if k < lay.core else every[j]
            if at:
                row = pltpu.roll(row, rank, 1)
            head[k] = jnp.where(lane < rank, row, msg[2 * k])
    tail = {k: msg[2 * k + 1] for k in head}
    for diff in range(lay.nb):
        base = (b ^ diff) * lay.rows_b
        k = lay.level_b(diff)
        send[base] = head[k]
        send[base + 1] = tail[k]
        send[base + 2] = core
    token[0] = core


def near_kernel(lay, start, near_src, count_src, far_src, pack, halo, after, *refs):
    del after
    head = start == HALO
    if head:
        p_ref, t_hbm, w_hbm, near_out, far_out, w_out, node_out, p_s = refs[:8]
        refs = refs[8:]
    else:
        t_hbm, near_out, far_out = refs[:3]
        refs = refs[3:]
    near_list, near_count, far_list, win, tgt, acc, t_ref, sem = refs
    leaves, lanes = near_out.shape[0], pack.shape[2]
    rank = lanes // 2
    tiles = lanes // 8
    far_tiles = rank // 8
    moves = [
        (near_src, near_list),
        (count_src, near_count),
        (far_src, far_list),
        (t_hbm.at[pl.ds(start, leaves)], t_ref),
    ]
    if head:
        moves.append((w_hbm, w_out))
    copies = [pltpu.make_async_copy(src, dst, sem.at[n]) for n, (src, dst) in enumerate(moves)]
    for copy in copies:
        copy.start()
    total = pack.shape[0]
    if start == 0:
        win[0:HALO] = halo[...]
    elif not head:
        win[HALO + total :] = halo[...]
    win[HALO : HALO + total] = pack[...]

    pick = lax.broadcasted_iota(jnp.int32, (32, 3 * lanes), 0) % 8
    wide = lax.broadcasted_iota(jnp.int32, (32, 3 * lanes), 1) // lanes
    choose = jnp.where(pick == wide, 1.0, 0.0).astype(jnp.bfloat16)
    used = lax.broadcasted_iota(jnp.int32, (8, lanes), 0) < 3

    def spread(i):
        x = jnp.where(used, win[HALO + start + i], 0.0)
        high = x.astype(jnp.bfloat16).astype(jnp.float32)
        rest = x - high
        mid = rest.astype(jnp.bfloat16).astype(jnp.float32)
        parts = jnp.concatenate([high, mid, rest - mid, jnp.zeros_like(x)], axis=0)
        out = lax.dot_general(
            parts.astype(jnp.bfloat16), choose, (((0,), (0,)), ((), ())), preferred_element_type=jnp.float32
        )
        return [out[:, c * lanes : (c + 1) * lanes] for c in range(3)]

    def keep(i, cols):
        for c in range(3):
            tgt[i, c] = cols[c]

    if head:
        for k in range(3 * lay.levels):
            p_s[k : k + 1, :] = p_ref[k]
        own = jnp.transpose(p_s[...])
        half = lax.broadcasted_iota(jnp.int32, (rank, lanes), 1) < rank
        for n, (one, two) in enumerate(lay.couples):
            for c in range(3):
                left, right = own[:, 3 * one + c : 3 * one + c + 1], own[:, 3 * two + c : 3 * two + c + 1]
                node_out[3 * n + c] = jnp.where(half, left, right)
    for i in range(UNROLL):
        keep(i, spread(i))
    for copy in copies[:3]:
        copy.wait()

    def weighted(i, t, xs):
        at = pl.ds(8 * t, 8)
        d0 = tgt[i, 0, at, :] - xs[0]
        d1 = tgt[i, 1, at, :] - xs[1]
        d2 = tgt[i, 2, at, :] - xs[2]
        return lax.rsqrt((d0 * d0 + d1 * d1 + d2 * d2) + SOFTENING) * xs[3]

    def rows(j, which):
        return [jnp.broadcast_to(win[j, pl.ds(r, 1), :], (8, lanes)) for r in which]

    lane = lax.broadcasted_iota(jnp.int32, (8, lanes), 1)

    def far_field(g, more):
        ahead = [spread((g + 1) * UNROLL + u) for u in range(UNROLL)] if more else []
        for u in range(UNROLL):
            i = g * UNROLL + u
            both = []
            for m in range(0, far_list.shape[0], 2):
                block = jnp.where(lane < rank, win[far_list[m, start + i]], win[far_list[m + 1, start + i]])
                both.append([jnp.broadcast_to(block[r : r + 1, :], (8, lanes)) for r in (5, 6, 7, 4)])
            for t in range(far_tiles):
                far = weighted(i, t, both[0])
                for xs in both[1:]:
                    far = far + weighted(i, t, xs)
                far_out[i, pl.ds(8 * t, 8), :] = far + pltpu.roll(far, rank, 1)
        for u, cols in enumerate(ahead):
            keep((g + 1) * UNROLL + u, cols)

    def far_step(g, carry):
        far_field(g, True)
        return carry

    groups = leaves // UNROLL
    lax.fori_loop(0, groups - 1, far_step, 0)
    far_field(groups - 1, False)

    def leaf(i, carry):
        count = near_count[start + i]
        for t in range(tiles):
            acc[i, pl.ds(8 * t, 8), :] = jnp.zeros((8, lanes), jnp.float32)

        def slots(n, inner):
            m = 2 * n + 1
            one = rows(near_list[m, start + i], range(4))
            then = jnp.minimum(m + 1, near_list.shape[0] - 1)
            two = rows(near_list[then, start + i], range(4))
            two[3] = two[3] * jnp.where(m + 1 < count, 1.0, 0.0)
            for t in range(tiles):
                at = pl.ds(8 * t, 8)
                acc[i, at, :] = acc[i, at, :] + (weighted(i, t, one) + weighted(i, t, two))
            return inner

        return lax.fori_loop(0, count // 2, slots, carry)

    lax.fori_loop(0, leaves, leaf, 0)
    copies[3].wait()

    def finish(i, carry):
        own = rows(near_list[0, start + i], range(4))
        sums = [acc[i, pl.ds(8 * t, 8), :] + weighted(i, t, own) for t in range(tiles)]
        whole = jnp.concatenate(sums, axis=0)
        near_out[i] = jnp.sum(jnp.transpose(whole), axis=0, keepdims=True)
        for t in range(far_tiles):
            at = pl.ds(8 * t, 8)
            tile = t_ref[i, at, :]
            far_out[i, at, :] = jnp.where(lane < rank, side(tile, tile), far_out[i, at, :])
        return carry

    lax.fori_loop(0, leaves, finish, 0, unroll=FINISH)
    for copy in copies[4:]:
        copy.wait()


def post_kernel(lay, recv_a, recv_b, f_ref, near1, far1, near, far, near2, far2, w_ref, node, out, row_s, up_s):
    rank = w_ref.shape[1]
    mask = eye(rank, rank)
    a, b = lay.place()
    got_a = lambda diff, r: recv_a[(a ^ diff) * lay.rows_a + r]
    got_b = lambda diff, r: recv_b[(b ^ diff) * lay.rows_b + r]

    weight, first = {}, {}
    for diff in range(1, lay.na):
        k = lay.level_a(diff)
        row = got_a(diff, 0)
        weight[k] = weight[k] + row if k in weight else row
        if k not in first:
            first[k] = (row, got_a(diff, 1))
    for diff in range(1, lay.nb):
        k = lay.level_b(diff)
        row = got_b(diff, 0)
        weight[k] = weight[k] + row if k in weight else row
        if k not in first:
            first[k] = (row, got_b(diff, 1))
        if diff < lay.ny:
            weight[lay.core] = weight[lay.core] + got_b(diff, 2)

    lane = lax.broadcasted_iota(jnp.int32, (1, 2 * rank), 1)
    turned = lambda x: pltpu.roll(x, rank, 1)
    value, carried = 0.0, 0.0
    for n, (one, two) in enumerate(lay.couples):
        (top, bottom), (top2, bottom2) = first[one], first[two]
        xs = [
            jnp.where(lane < rank, turned(top), top2),
            jnp.where(lane < rank, bottom, turned(bottom2)),
            jnp.where(lane < rank, turned(bottom), bottom2),
        ]
        amount = jnp.where(lane < rank, weight[one], turned(weight[two]))
        squares = 0.0
        for c in range(3):
            d = node[3 * n + c] - xs[c]
            squares = squares + d * d
        terms = lax.rsqrt(squares + SOFTENING) * amount
        for k in (one,) if one == two else (one, two):
            keep = lane < rank if k == one else lane >= rank
            col = jnp.sum(jnp.where(keep, terms, 0.0), axis=1, keepdims=True)
            if k:
                carried = carried + f_ref[k - 1] * to_row(col, mask)
            else:
                value = col
    value = value + jnp.sum(carried, axis=1, keepdims=True)
    row = jnp.where(lane < rank, to_row(value, eye(rank, 2 * rank)), 1.0)

    where = [
        (parts, i) for parts in ((near1, far1), (near, far), (near2, far2)) for i in range(parts[1].shape[0])
    ]
    for i, (parts, at) in enumerate(where):
        col = jnp.sum(parts[1][at] * row, axis=1, keepdims=True)
        row_s[i : i + 1, :] = to_row(col, mask)
        up_s[i : i + 1, :] = jnp.sum(w_ref[i] * col, axis=0, keepdims=True)
    for i, (parts, at) in enumerate(where):
        out[i : i + 1, :] = parts[0][at]
    out[...] = out[...] + side(row_s[...], up_s[...])


def in_vmem(x):
    return x if INTERPRET else pltpu.with_memory_space_constraint(x, pltpu.VMEM)


def in_hbm(x):
    return x if INTERPRET else pltpu.with_memory_space_constraint(x, pltpu.HBM)


def made(shape, dtype=jnp.float32):
    return jax.ShapeDtypeStruct(shape, dtype) if INTERPRET else pltpu.VMEM(shape, dtype)


def call(body, in_specs, outs, scratch, flops=0):
    kwargs = {"interpret": True} if INTERPRET else {}
    return pl.pallas_call(
        body,
        in_specs=in_specs,
        out_specs=tuple(pl.BlockSpec(memory_space=pltpu.VMEM) for _ in outs),
        out_shape=tuple(outs),
        scratch_shapes=scratch,
        compiler_params=pltpu.CompilerParams(vmem_limit_bytes=32 << 20),
        cost_estimate=pl.CostEstimate(flops=flops, transcendentals=0, bytes_accessed=1 << 16) if flops else None,
        **kwargs,
    )


VM = pl.BlockSpec(memory_space=pltpu.VMEM)
SM = pl.BlockSpec(memory_space=pltpu.SMEM)
HB = pl.BlockSpec(memory_space=pl.ANY if INTERPRET else pltpu.HBM)


def POST_IN():
    return [VM] * 11


def POST_SCRATCH(leaves, rank):
    return [
        pltpu.VMEM((leaves, rank), jnp.float32),
        pltpu.VMEM((leaves, rank), jnp.float32),
    ]


def on_device(
    lay,
    points,
    charges,
    interpolant,
    leaf_transfer,
    node_transfer,
    node_points,
    near_list,
    near_count,
    far_list,
):
    leaves, rank = interpolant.shape[0], interpolant.shape[1]
    lanes = points.shape[2]
    levels = lay.levels
    pts = jnp.transpose(points, (1, 0, 2))
    transfers = node_transfer[0]
    centres = jnp.transpose(node_points, (1, 2, 0, 3)).reshape(3 * levels, 1, rank)
    tables = (near_list.T, near_count, far_list.T)
    vec = lambda n: made((n, 1, lanes))

    pack, lo, hi, send, msg, f_ref, p_ref, *lists = call_pre(
        lay, pts, charges, centres, transfers, interpolant, leaf_transfer, tables
    )

    recv_a = lax.all_to_all(send, AXES, 0, 0, axis_index_groups=lay.groups_a(), tiled=True)
    near, far, w_ref, node = near_call(
        lay, HALO, leaves - 2 * HALO, lists, pack, lo, hi, p_ref, leaf_transfer, interpolant
    )
    count = lay.na * lay.nb
    up = [(i, i + 1) for i in range(count - 1)]
    low = lax.ppermute(hi, AXES, up)
    high = lax.ppermute(lo, AXES, [(b, a) for a, b in up])

    send_b, token = call(
        lambda *refs: mid_kernel(lay, *refs), [VM, VM], [vec(lay.nb * lay.rows_b), vec(1)], []
    )(in_vmem(recv_a), in_vmem(msg))
    recv_b = lax.all_to_all(send_b, AXES, 0, 0, axis_index_groups=lay.groups_b(), tiled=True)

    near1, far1 = near_call(lay, 0, HALO, lists, pack, low, token, p_ref, leaf_transfer, interpolant)
    near2, far2 = near_call(
        lay, leaves - HALO, HALO, lists, pack, high, near1, p_ref, leaf_transfer, interpolant
    )

    (out,) = call(
        lambda *refs: post_kernel(lay, *refs),
        POST_IN(),
        [jax.ShapeDtypeStruct((leaves, lanes), jnp.float32)],
        POST_SCRATCH(leaves, rank),
    )(*(in_vmem(x) for x in (recv_a, recv_b, f_ref, near1, far1, near, far, near2, far2, w_ref, node)))
    return out


def call_pre(lay, pts, charges, centres, transfers, interpolant, leaf_transfer, tables):
    leaves, rank = interpolant.shape[0], interpolant.shape[1]
    lanes = charges.shape[1]
    levels = lay.levels
    vec = lambda n: made((n, 1, lanes))
    return call(
        lambda *refs: pre_kernel(lay, *refs),
        [HB] * 9,
        [
            made((leaves, 8, lanes)),
            made((HALO, 8, lanes)),
            made((HALO, 8, lanes)),
            vec(lay.na * lay.rows_a),
            vec(2 * levels),
            made((levels - 1, rank, rank)),
            made((3 * levels, 1, rank)),
            *(made(x.shape, jnp.int32) for x in tables),
        ],
        [
            pltpu.VMEM((3, leaves, lanes), jnp.float32),
            pltpu.VMEM((leaves, lanes), jnp.float32),
            pltpu.VMEM((leaves, rank, rank), jnp.float32),
            pltpu.VMEM((leaves, rank, rank), jnp.float32),
            pltpu.VMEM((levels, rank, rank), jnp.float32),
            pltpu.SemaphoreType.DMA((2 * CHUNKS + 7,)),
        ],
    )(*(in_hbm(x) for x in (pts, charges, centres, transfers, interpolant, leaf_transfer, *tables)))


def near_call(lay, start, leaves, lists, pack, halo, token, p_ref, leaf_transfer, interpolant):
    total, rank = interpolant.shape[0], interpolant.shape[1]
    lanes = pack.shape[2]
    head = start == HALO
    outs = [made((leaves, 1, lanes)), made((leaves, rank, lanes))]
    extra = []
    if head:
        outs += [made((total, rank, rank)), made((3 * len(lay.couples), rank, lanes))]
        extra = [pltpu.VMEM((-(-3 * lay.levels // 8) * 8, rank), jnp.float32)]
    near_inputs = [*lists, pack, halo, token] + ([p_ref] if head else [])
    far_inputs = [leaf_transfer] + ([interpolant] if head else [])
    return call(
        lambda *refs: near_kernel(lay, start, *refs),
        [VM] * len(near_inputs) + [HB] * len(far_inputs),
        outs,
        [
            *extra,
            *(pltpu.SMEM(x.shape, jnp.int32) for x in lists),
            pltpu.VMEM((total + 2 * HALO, 8, lanes), jnp.float32),
            pltpu.VMEM((leaves, 3, lanes, lanes), jnp.float32),
            pltpu.VMEM((leaves, lanes, lanes), jnp.float32),
            pltpu.VMEM((leaves, rank, rank), jnp.float32),
            pltpu.SemaphoreType.DMA((5,)),
        ],
        flops=200_000_000,
    )(*(in_vmem(x) for x in near_inputs), *(in_hbm(x) for x in far_inputs))


def solution(mesh):
    lay = Layout(*(mesh.shape[name] for name in AXES))
    split = lambda rest: P(AXES, *([None] * rest))

    def body(*args):
        return on_device(lay, *args)

    return jax.shard_map(
        body,
        mesh=mesh,
        in_specs=(split(2), split(1), split(2), split(2), split(3), split(3), split(1), split(0), split(1)),
        out_specs=split(1),
        check_vma=False,
    )
```

```python
import jax
import jax.numpy as jnp
from jax import lax
from jax.experimental import pallas as pl
from jax.experimental.pallas import tpu as pltpu
from jax.sharding import PartitionSpec as P


HALO = 8
SOFTENING = 0.0625
AXES = ("gx", "gy", "gz")
INTERPRET = False
CHUNKS = 4
UNROLL = 8
FINISH = 8


class Layout:
    def __init__(self, nx, ny, nz):
        self.nx, self.ny, self.nz = nx, ny, nz
        self.bx, self.by, self.bz = (n.bit_length() - 1 for n in (nx, ny, nz))
        self.levels = self.bx + self.by + self.bz
        self.core = self.bz + self.by
        self.na = 2 * nz
        self.nb = (nx // 2) * ny
        self.low = list(range(self.bz, self.core))
        self.high = list(range(self.core + 1, self.levels))
        both = self.low + self.high
        self.pairs = [both[i : i + 2] for i in range(0, len(both), 2)]
        self.rows_a = 2 + len(self.pairs)
        self.rows_b = 3
        self.couples = [(k, min(k + 1, self.levels - 1)) for k in range(0, self.levels, 2)]

    def device(self, a, b):
        gz, core = a % self.nz, a // self.nz
        gy, up = b % self.ny, b // self.ny
        return ((up * 2 + core) * self.ny + gy) * self.nz + gz

    def groups_a(self):
        return [[self.device(a, b) for a in range(self.na)] for b in range(self.nb)]

    def groups_b(self):
        return [[self.device(a, b) for b in range(self.nb)] for a in range(self.na)]

    def level_a(self, diff):
        if diff == 0:
            return 0
        return self.core if diff >= self.nz else diff.bit_length() - 1

    def level_b(self, diff):
        high, low = diff // self.ny, diff % self.ny
        if high:
            return self.core + high.bit_length()
        return self.bz + low.bit_length() - 1 if low else self.bz

    def place(self):
        gx, gy, gz = (lax.axis_index(name) for name in AXES)
        return (gx % 2) * self.nz + gz, (gx // 2) * self.ny + gy


def eye(rows, lanes):
    r = lax.broadcasted_iota(jnp.int32, (rows, lanes), 0)
    c = lax.broadcasted_iota(jnp.int32, (rows, lanes), 1)
    return r == c % rows


def to_row(col, mask):
    return jnp.sum(jnp.where(mask, col, 0.0), axis=0, keepdims=True)


def product(x, y):
    return jnp.dot(x, y, precision=lax.Precision.HIGHEST, preferred_element_type=jnp.float32)


def side(left, right):
    return jnp.concatenate([left, right], axis=1)


def pre_kernel(
    lay, pts_hbm, q_hbm, p_hbm, e_hbm, w_hbm, t_hbm, l1_hbm, l2_hbm, l3_hbm,
    pack, lo, hi, send, msg, f_ref, p_ref, l1, l2, l3, pts, q, w_ref, t_ref, e_ref, sem,
):
    leaves, rank = w_ref.shape[0], w_ref.shape[1]
    step = leaves // CHUNKS
    small = [
        pltpu.make_async_copy(src, dst, sem.at[2 * CHUNKS + n])
        for n, (src, dst) in enumerate((
            (q_hbm, q),
            (pts_hbm, pts),
            (e_hbm, e_ref),
            (p_hbm, p_ref),
            (l1_hbm, l1),
            (l2_hbm, l2),
            (l3_hbm, l3),
        )
        )
    ]
    for copy in small[:3]:
        copy.start()
    copies = []
    for c in range(CHUNKS):
        part = pl.ds(c * step, step)
        copies.append(
            (
                pltpu.make_async_copy(w_hbm.at[part], w_ref.at[part], sem.at[2 * c]),
                pltpu.make_async_copy(t_hbm.at[part], t_ref.at[part], sem.at[2 * c + 1]),
            )
        )
    for w_copy, t_copy in copies:
        w_copy.start()
        t_copy.start()
    for copy in small[3:]:
        copy.start()
    small[0].wait()
    small[1].wait()

    mask = eye(rank, rank)
    mask2 = eye(rank, 2 * rank)
    lane = lax.broadcasted_iota(jnp.int32, (leaves, 2 * rank), 1)
    charge = q[...]
    coords = [pts[c] for c in range(3)]
    twice = [jnp.where(lane < rank, x, pltpu.roll(x, rank, 1)) for x in coords]
    other = pltpu.roll(charge, rank, 1)
    for i in range(leaves):
        for r, x in ((0, coords[0]), (1, coords[1]), (2, coords[2]), (3, charge)):
            pack[i, r : r + 1, :] = x[i : i + 1, :]
        for r in range(3):
            pack[i, 5 + r : 6 + r, :] = twice[r][i : i + 1, :]

    assert lay.levels <= 2 * CHUNKS + 1
    total = jnp.zeros((rank, rank), jnp.float32)
    for c in range(CHUNKS):
        copies[c][0].wait()
        copies[c][1].wait()
        if c == 0:
            small[2].wait()
            f_ref[0] = e_ref[0]
            doubles = {k: product(e_ref[k], e_ref[k + 1]) for k in range(0, lay.levels - 2, 2)}
            if doubles:
                f_ref[1] = doubles[0]
        else:
            for k in (2 * c, 2 * c + 1):
                if k < lay.levels - 1:
                    f_ref[k] = product(f_ref[2 * c - 1], doubles[k - 1] if k % 2 else e_ref[k])
        for i in range(c * step, (c + 1) * step):
            own = jnp.where(mask, charge[i : i + 1, :rank], 0.0)
            col = jnp.sum(w_ref[i] * other[i : i + 1, :rank] + own, axis=1, keepdims=True)
            total = total + t_ref[i] * col
            pack[i, 4:5, :] = to_row(col, mask2)
    first = jnp.where(lax.axis_index("gz") % 2 == 0, leaves - HALO, 0)
    lo[...] = pack[pl.ds(first, HALO)]
    hi[...] = pack[pl.ds(leaves - HALO - first, HALO)]
    for copy in small[3:]:
        copy.wait()

    rows = [jnp.sum(total, axis=0, keepdims=True)]
    col = jnp.sum(jnp.where(mask, rows[0], 0.0), axis=1, keepdims=True)
    for k in range(1, lay.levels):
        rows.append(jnp.sum(f_ref[k - 1] * col, axis=0, keepdims=True))

    head = [side(rows[k], p_ref[3 * k]) for k in range(lay.levels)]
    tail = [side(p_ref[3 * k + 1], p_ref[3 * k + 2]) for k in range(lay.levels)]
    sums = [side(rows[pair[0]], rows[pair[-1]]) for pair in lay.pairs]
    for k in range(lay.levels):
        msg[2 * k] = head[k]
        msg[2 * k + 1] = tail[k]
    a, _ = lay.place()
    for diff in range(lay.na):
        base = (a ^ diff) * lay.rows_a
        k = lay.level_a(diff)
        for r, row in enumerate([head[k], tail[k]] + sums):
            send[base + r] = row


def gathered_a(lay, recv, a):
    near, every = [], []
    for j in range(len(lay.pairs)):
        rows = [recv[(a ^ diff) * lay.rows_a + 2 + j] for diff in range(lay.na)]
        part = sum(rows[1 : lay.nz], rows[0])
        near.append(part)
        every.append(sum(rows[lay.nz + 1 :], rows[lay.nz]) + part)
    core = [recv[(a ^ diff) * lay.rows_a] for diff in range(lay.nz, lay.na)]
    return near, every, sum(core[1:], core[0])


def mid_kernel(lay, recv, msg, send, token):
    rank = msg.shape[2] // 2
    a, b = lay.place()
    near, every, core = gathered_a(lay, recv, a)
    lane = lax.broadcasted_iota(jnp.int32, (1, 2 * rank), 1)
    head = {}
    for j, pair in enumerate(lay.pairs):
        for at, k in enumerate(pair):
            row = near[j] if k < lay.core else every[j]
            if at:
                row = pltpu.roll(row, rank, 1)
            head[k] = jnp.where(lane < rank, row, msg[2 * k])
    tail = {k: msg[2 * k + 1] for k in head}
    for diff in range(lay.nb):
        base = (b ^ diff) * lay.rows_b
        k = lay.level_b(diff)
        send[base] = head[k]
        send[base + 1] = tail[k]
        send[base + 2] = core
    token[0] = core


def near_kernel(lay, head, near_src, count_src, far_src, pack, *refs):
    if head:
        _, p_ref, t_hbm, w_hbm, near_out, far_out, w_out, node_out, p_s = refs[:9]
        refs = refs[9:]
    else:
        one, two, _, t_hbm, near_out, far_out = refs[:6]
        refs = refs[6:]
    near_list, near_count, far_list, win, tgt, acc, t_ref, sem = refs
    leaves, lanes = near_out.shape[0], pack.shape[2]
    rank = lanes // 2
    tiles = lanes // 8
    far_tiles = rank // 8
    moves = [
        (near_src, near_list),
        (count_src, near_count),
        (far_src, far_list),
    ]
    total = pack.shape[0]
    if head:
        moves.append((t_hbm.at[pl.ds(HALO, leaves)], t_ref))
        moves.append((w_hbm, w_out))
    else:
        moves.append((t_hbm.at[pl.ds(0, HALO)], t_ref.at[pl.ds(0, HALO)]))
        moves.append((t_hbm.at[pl.ds(total - HALO, HALO)], t_ref.at[pl.ds(HALO, HALO)]))
    copies = [pltpu.make_async_copy(src, dst, sem.at[n]) for n, (src, dst) in enumerate(moves)]
    for copy in copies:
        copy.start()
    if not head:
        even = lax.axis_index("gz") % 2 == 0
        win[0:HALO] = jnp.where(even, two[...], one[...])
        win[HALO + total :] = jnp.where(even, one[...], two[...])

    def name(i):
        return HALO + i if head else i + (i // HALO) * (total - 2 * HALO)

    win[HALO : HALO + total] = pack[...]

    pick = lax.broadcasted_iota(jnp.int32, (32, 3 * lanes), 0) % 8
    wide = lax.broadcasted_iota(jnp.int32, (32, 3 * lanes), 1) // lanes
    choose = jnp.where(pick == wide, 1.0, 0.0).astype(jnp.bfloat16)
    used = lax.broadcasted_iota(jnp.int32, (8, lanes), 0) < 3

    def spread(i):
        x = jnp.where(used, win[HALO + name(i)], 0.0)
        high = x.astype(jnp.bfloat16).astype(jnp.float32)
        rest = x - high
        mid = rest.astype(jnp.bfloat16).astype(jnp.float32)
        parts = jnp.concatenate([high, mid, rest - mid, jnp.zeros_like(x)], axis=0)
        out = lax.dot_general(
            parts.astype(jnp.bfloat16), choose, (((0,), (0,)), ((), ())), preferred_element_type=jnp.float32
        )
        return [out[:, c * lanes : (c + 1) * lanes] for c in range(3)]

    def keep(i, cols):
        for c in range(3):
            tgt[i, c] = cols[c]

    if head:
        for k in range(3 * lay.levels):
            p_s[k : k + 1, :] = p_ref[k]
        own = jnp.transpose(p_s[...])
        half = lax.broadcasted_iota(jnp.int32, (rank, lanes), 1) < rank
        for n, (one, two) in enumerate(lay.couples):
            for c in range(3):
                left, right = own[:, 3 * one + c : 3 * one + c + 1], own[:, 3 * two + c : 3 * two + c + 1]
                node_out[3 * n + c] = jnp.where(half, left, right)
    for i in range(UNROLL):
        keep(i, spread(i))
    for copy in copies[:3]:
        copy.wait()

    def weighted(i, t, xs):
        at = pl.ds(8 * t, 8)
        d0 = tgt[i, 0, at, :] - xs[0]
        d1 = tgt[i, 1, at, :] - xs[1]
        d2 = tgt[i, 2, at, :] - xs[2]
        return lax.rsqrt((d0 * d0 + d1 * d1 + d2 * d2) + SOFTENING) * xs[3]

    def rows(j, which):
        return [jnp.broadcast_to(win[j, pl.ds(r, 1), :], (8, lanes)) for r in which]

    lane = lax.broadcasted_iota(jnp.int32, (8, lanes), 1)

    def far_field(g, more):
        ahead = [spread((g + 1) * UNROLL + u) for u in range(UNROLL)] if more else []
        for u in range(UNROLL):
            i = g * UNROLL + u
            both = []
            for m in range(0, far_list.shape[0], 2):
                block = jnp.where(lane < rank, win[far_list[m, name(i)]], win[far_list[m + 1, name(i)]])
                both.append([jnp.broadcast_to(block[r : r + 1, :], (8, lanes)) for r in (5, 6, 7, 4)])
            for t in range(far_tiles):
                far = weighted(i, t, both[0])
                for xs in both[1:]:
                    far = far + weighted(i, t, xs)
                far_out[i, pl.ds(8 * t, 8), :] = far + pltpu.roll(far, rank, 1)
        for u, cols in enumerate(ahead):
            keep((g + 1) * UNROLL + u, cols)

    def far_step(g, carry):
        far_field(g, True)
        return carry

    groups = leaves // UNROLL
    lax.fori_loop(0, groups - 1, far_step, 0)
    far_field(groups - 1, False)

    def leaf(i, carry):
        count = near_count[name(i)]
        for t in range(tiles):
            acc[i, pl.ds(8 * t, 8), :] = jnp.zeros((8, lanes), jnp.float32)

        def slots(n, inner):
            m = 2 * n + 1
            one = rows(near_list[m, name(i)], range(4))
            then = jnp.minimum(m + 1, near_list.shape[0] - 1)
            two = rows(near_list[then, name(i)], range(4))
            two[3] = two[3] * jnp.where(m + 1 < count, 1.0, 0.0)
            for t in range(tiles):
                at = pl.ds(8 * t, 8)
                acc[i, at, :] = acc[i, at, :] + (weighted(i, t, one) + weighted(i, t, two))
            return inner

        return lax.fori_loop(0, count // 2, slots, carry)

    lax.fori_loop(0, leaves, leaf, 0)
    for copy in copies[3:]:
        copy.wait()

    def finish(i, carry):
        own = rows(near_list[0, name(i)], range(4))
        sums = [acc[i, pl.ds(8 * t, 8), :] + weighted(i, t, own) for t in range(tiles)]
        whole = jnp.concatenate(sums, axis=0)
        near_out[i] = jnp.sum(jnp.transpose(whole), axis=0, keepdims=True)
        for t in range(far_tiles):
            at = pl.ds(8 * t, 8)
            tile = t_ref[i, at, :]
            far_out[i, at, :] = jnp.where(lane < rank, side(tile, tile), far_out[i, at, :])
        return carry

    lax.fori_loop(0, leaves, finish, 0, unroll=FINISH)


def post_kernel(lay, recv_a, recv_b, f_ref, near1, far1, near, far, w_ref, node, out, row_s, up_s):
    leaves, rank = w_ref.shape[0], w_ref.shape[1]
    mask = eye(rank, rank)
    a, b = lay.place()
    got_a = lambda diff, r: recv_a[(a ^ diff) * lay.rows_a + r]
    got_b = lambda diff, r: recv_b[(b ^ diff) * lay.rows_b + r]

    weight, first = {}, {}
    for diff in range(1, lay.na):
        k = lay.level_a(diff)
        row = got_a(diff, 0)
        weight[k] = weight[k] + row if k in weight else row
        if k not in first:
            first[k] = (row, got_a(diff, 1))
    for diff in range(1, lay.nb):
        k = lay.level_b(diff)
        row = got_b(diff, 0)
        weight[k] = weight[k] + row if k in weight else row
        if k not in first:
            first[k] = (row, got_b(diff, 1))
        if diff < lay.ny:
            weight[lay.core] = weight[lay.core] + got_b(diff, 2)

    lane = lax.broadcasted_iota(jnp.int32, (1, 2 * rank), 1)
    turned = lambda x: pltpu.roll(x, rank, 1)
    value, carried = 0.0, 0.0
    for n, (one, two) in enumerate(lay.couples):
        (top, bottom), (top2, bottom2) = first[one], first[two]
        xs = [
            jnp.where(lane < rank, turned(top), top2),
            jnp.where(lane < rank, bottom, turned(bottom2)),
            jnp.where(lane < rank, turned(bottom), bottom2),
        ]
        amount = jnp.where(lane < rank, weight[one], turned(weight[two]))
        squares = 0.0
        for c in range(3):
            d = node[3 * n + c] - xs[c]
            squares = squares + d * d
        terms = lax.rsqrt(squares + SOFTENING) * amount
        for k in (one,) if one == two else (one, two):
            keep = lane < rank if k == one else lane >= rank
            col = jnp.sum(jnp.where(keep, terms, 0.0), axis=1, keepdims=True)
            if k:
                carried = carried + f_ref[k - 1] * to_row(col, mask)
            else:
                value = col
    value = value + jnp.sum(carried, axis=1, keepdims=True)
    row = jnp.where(lane < rank, to_row(value, eye(rank, 2 * rank)), 1.0)

    ends, inside = (near1, far1), (near, far)
    where = [(ends, i) for i in range(HALO)] + [(inside, i) for i in range(leaves - 2 * HALO)]
    where += [(ends, HALO + i) for i in range(HALO)]
    for i, (parts, at) in enumerate(where):
        col = jnp.sum(parts[1][at] * row, axis=1, keepdims=True)
        row_s[i : i + 1, :] = to_row(col, mask)
        up_s[i : i + 1, :] = jnp.sum(w_ref[i] * col, axis=0, keepdims=True)
    for i, (parts, at) in enumerate(where):
        out[i : i + 1, :] = parts[0][at]
    out[...] = out[...] + side(row_s[...], up_s[...])


def in_vmem(x):
    return x if INTERPRET else pltpu.with_memory_space_constraint(x, pltpu.VMEM)


def in_hbm(x):
    return x if INTERPRET else pltpu.with_memory_space_constraint(x, pltpu.HBM)


def made(shape, dtype=jnp.float32):
    return jax.ShapeDtypeStruct(shape, dtype) if INTERPRET else pltpu.VMEM(shape, dtype)


def call(body, in_specs, outs, scratch, flops=0):
    kwargs = {"interpret": True} if INTERPRET else {}
    return pl.pallas_call(
        body,
        in_specs=in_specs,
        out_specs=tuple(pl.BlockSpec(memory_space=pltpu.VMEM) for _ in outs),
        out_shape=tuple(outs),
        scratch_shapes=scratch,
        compiler_params=pltpu.CompilerParams(vmem_limit_bytes=32 << 20),
        cost_estimate=pl.CostEstimate(flops=flops, transcendentals=0, bytes_accessed=1 << 16) if flops else None,
        **kwargs,
    )


VM = pl.BlockSpec(memory_space=pltpu.VMEM)
SM = pl.BlockSpec(memory_space=pltpu.SMEM)
HB = pl.BlockSpec(memory_space=pl.ANY if INTERPRET else pltpu.HBM)


def POST_IN():
    return [VM] * 9


def POST_SCRATCH(leaves, rank):
    return [
        pltpu.VMEM((leaves, rank), jnp.float32),
        pltpu.VMEM((leaves, rank), jnp.float32),
    ]


def on_device(
    lay,
    points,
    charges,
    interpolant,
    leaf_transfer,
    node_transfer,
    node_points,
    near_list,
    near_count,
    far_list,
):
    leaves, rank = interpolant.shape[0], interpolant.shape[1]
    lanes = points.shape[2]
    levels = lay.levels
    pts = jnp.transpose(points, (1, 0, 2))
    transfers = node_transfer[0]
    centres = jnp.transpose(node_points, (1, 2, 0, 3)).reshape(3 * levels, 1, rank)
    tables = (near_list.T, near_count, far_list.T)
    vec = lambda n: made((n, 1, lanes))

    pack, lo, hi, send, msg, f_ref, p_ref, *lists = call_pre(
        lay, pts, charges, centres, transfers, interpolant, leaf_transfer, tables
    )

    recv_a = lax.all_to_all(send, AXES, 0, 0, axis_index_groups=lay.groups_a(), tiled=True)
    count = lay.na * lay.nb
    one = lax.ppermute(lo, AXES, [(i, i ^ 1) for i in range(count)])
    links = [(i, i + 1) for i in range(1, count - 1, 2)]
    two = lax.ppermute(hi, AXES, links + [(j, i) for i, j in links])

    send_b, token = call(
        lambda *refs: mid_kernel(lay, *refs), [VM, VM], [vec(lay.nb * lay.rows_b), vec(1)], []
    )(in_vmem(recv_a), in_vmem(msg))
    recv_b = lax.all_to_all(send_b, AXES, 0, 0, axis_index_groups=lay.groups_b(), tiled=True)

    near, far, w_ref, node = near_call(
        lay, True, lists, pack, (token, p_ref), leaf_transfer, interpolant
    )
    near1, far1 = near_call(lay, False, lists, pack, (one, two, near), leaf_transfer, interpolant)

    (out,) = call(
        lambda *refs: post_kernel(lay, *refs),
        POST_IN(),
        [jax.ShapeDtypeStruct((leaves, lanes), jnp.float32)],
        POST_SCRATCH(leaves, rank),
    )(*(in_vmem(x) for x in (recv_a, recv_b, f_ref, near1, far1, near, far, w_ref, node)))
    return out


def call_pre(lay, pts, charges, centres, transfers, interpolant, leaf_transfer, tables):
    leaves, rank = interpolant.shape[0], interpolant.shape[1]
    lanes = charges.shape[1]
    levels = lay.levels
    vec = lambda n: made((n, 1, lanes))
    return call(
        lambda *refs: pre_kernel(lay, *refs),
        [HB] * 9,
        [
            made((leaves, 8, lanes)),
            made((HALO, 8, lanes)),
            made((HALO, 8, lanes)),
            vec(lay.na * lay.rows_a),
            vec(2 * levels),
            made((levels - 1, rank, rank)),
            made((3 * levels, 1, rank)),
            *(made(x.shape, jnp.int32) for x in tables),
        ],
        [
            pltpu.VMEM((3, leaves, lanes), jnp.float32),
            pltpu.VMEM((leaves, lanes), jnp.float32),
            pltpu.VMEM((leaves, rank, rank), jnp.float32),
            pltpu.VMEM((leaves, rank, rank), jnp.float32),
            pltpu.VMEM((levels, rank, rank), jnp.float32),
            pltpu.SemaphoreType.DMA((2 * CHUNKS + 7,)),
        ],
    )(*(in_hbm(x) for x in (pts, charges, centres, transfers, interpolant, leaf_transfer, *tables)))


def near_call(lay, head, lists, pack, others, leaf_transfer, interpolant):
    total, rank = interpolant.shape[0], interpolant.shape[1]
    lanes = pack.shape[2]
    leaves = total - 2 * HALO if head else 2 * HALO
    outs = [made((leaves, 1, lanes)), made((leaves, rank, lanes))]
    extra = []
    if head:
        outs += [made((total, rank, rank)), made((3 * len(lay.couples), rank, lanes))]
        extra = [pltpu.VMEM((-(-3 * lay.levels // 8) * 8, rank), jnp.float32)]
    near_inputs = [*lists, pack, *others]
    far_inputs = [leaf_transfer] + ([interpolant] if head else [])
    return call(
        lambda *refs: near_kernel(lay, head, *refs),
        [VM] * len(near_inputs) + [HB] * len(far_inputs),
        outs,
        [
            *extra,
            *(pltpu.SMEM(x.shape, jnp.int32) for x in lists),
            pltpu.VMEM((total + 2 * HALO, 8, lanes), jnp.float32),
            pltpu.VMEM((leaves, 3, lanes, lanes), jnp.float32),
            pltpu.VMEM((leaves, lanes, lanes), jnp.float32),
            pltpu.VMEM((leaves, rank, rank), jnp.float32),
            pltpu.SemaphoreType.DMA((5,)),
        ],
        flops=200_000_000,
    )(*(in_vmem(x) for x in near_inputs), *(in_hbm(x) for x in far_inputs))


def solution(mesh):
    lay = Layout(*(mesh.shape[name] for name in AXES))
    split = lambda rest: P(AXES, *([None] * rest))

    def body(*args):
        return on_device(lay, *args)

    return jax.shard_map(
        body,
        mesh=mesh,
        in_specs=(split(2), split(1), split(2), split(2), split(3), split(3), split(1), split(0), split(1)),
        out_specs=split(1),
        check_vma=False,
    )
```
